256 devices in a mesh: shots: 4 (over y, x), gx: 32 (over z), gy: 2 (over core).
Axes of the slice: x: 2, y: 2, z: 32, core: 2. Of those that a mesh axis runs over, the one named last changes fastest.
The devices are a block of a 4x8x32 slice.
Arguments:
- pressure: float32 [128, 1024, 256], P(None, ('shots', 'gx'), 'gy'), parts along dimension 1, may hold values from -6 to 6
- pressure_prior: float32 [128, 1024, 256], P(None, ('shots', 'gx'), 'gy'), parts along dimension 1, may hold values from -6 to 6
- courant_square: bfloat16 [128, 256, 256], P(None, 'gx', 'gy'), may hold values from 0.049804688 to 0.1796875
- wavelet: float32 [64], P('shots'), parts along dimension 0, may hold values from -4 to 4
- delay_steps: int32 [1024, 256], P(('shots', 'gx'), 'gy'), parts along dimension 0, may hold values from 0 to 7
- source_depth: int32 [1024, 256], P(('shots', 'gx'), 'gy'), parts along dimension 0, may hold values from 4 to 31
- receiver_depth: int32 [1024, 256], P(('shots', 'gx'), 'gy'), parts along dimension 0, may hold values from 0 to 31
- receiver_field: float32 [128, 1024, 256], P(None, ('shots', 'gx'), 'gy'), parts along dimension 1, may hold values from -6 to 6
Outputs:
- pressure_final: float32 [128, 1024, 256], P(None, ('shots', 'gx'), 'gy'), parts along dimension 1
- image: float32 [128, 1024, 256], P('gx', 'shots', 'gy'), parts along dimension 1
The draws below stay inside these ranges and needn't reach their ends.
There are 4 independent parts, one for each index of `shots`. The reference program is written for one: setup_inputs(seed, part) draws one part's arguments, and reference() takes and returns one part's arrays. A program takes and returns all parts, laid end to end along the dimension named above; an argument that names none is the same for every part. Nothing has to cross between parts.
All inputs are finite; a program needn't handle non-finite values.
Results may differ from the reference program's by a relative error of at most 0.00035.
Values sent between devices are 32-bit elements; how exact they have to be, the bound alone decides.
No kernel may reach another device: no remote copies, remote signals or barrier semaphores. Data moves between devices by JAX's collectives and lax.ppermute only.
A program may use at most 64 MiB of HBM per device.

```python
import math
import jax
import jax.numpy as jnp

STEPS = 8
DMAX = 8
WAVE = 16
NX = 256
NY = 256
NZ = 128


def plant(array, stream_key, low, top_value):
    shape = array.shape
    spot = [jax.random.randint(jax.random.fold_in(stream_key, axis), (), 0, shape[axis]) for axis in range(len(shape))]
    array = array.at[tuple(spot)].set(low)
    longest = shape.index(max(shape))
    spot[longest] = (spot[longest] + 1) % shape[longest]
    return array.at[tuple(spot)].set(top_value)


def block_levels(rng, dims, cuts, low, high):
    def one(axis_at, parts):
        steps = jax.random.uniform(jax.random.fold_in(jax.random.fold_in(rng, 6), axis_at), (parts,), jnp.float32, low / len(cuts), high / len(cuts))
        return jnp.repeat(jnp.exp(steps), dims[axis_at] // parts).reshape((-1,) + (1,) * (len(dims) - axis_at - 1))

    factor_of = one(*cuts[0])
    for cut in cuts[1:]:
        factor_of = factor_of * one(*cut)
    return factor_of


def gaussian(key, dims, scale, most, split=(), kind=jnp.bfloat16):
    gain = block_levels(key, dims, split, -0.22, 0.18) if split else 1.0
    entries = jax.random.normal(key, dims, jnp.float32) * scale * gain
    return jnp.minimum(jnp.maximum(entries, -most), most).astype(kind)


def setup_inputs(seed: int = 0, part: int = 0) -> dict:
    seeds = jax.random.split(jax.random.key(seed), 9)
    own_keys = jax.random.split(jax.random.fold_in(seeds[8], part), 9)
    pressure = gaussian(own_keys[0], (NZ, NX, NY), 1.0, 6.0, ((1, 32), (2, 2)), jnp.float32)
    pressure_prior = gaussian(own_keys[1], (NZ, NX, NY), 1.0, 6.0, ((1, 32), (2, 2)), jnp.float32)
    courant_square = jnp.clip(jnp.exp(math.log(0.1796875) - 1.2831101 * jax.random.uniform(seeds[2], (NZ, NX, NY), jnp.float32) ** block_levels(seeds[2], (NZ, NX, NY), ((1, 32), (2, 2)), -0.2, 0.2)), 0.049804688, 0.1796875).astype(jnp.bfloat16)
    wavelet = gaussian(own_keys[3], (WAVE,), 1.0, 4.0, (), jnp.float32)
    delay_steps = plant(jax.random.randint(own_keys[4], (NX, NY), 0, DMAX), jax.random.fold_in(own_keys[4], 1), 0, DMAX - 1).astype(jnp.int32)
    source_depth = plant(jax.random.randint(own_keys[5], (NX, NY), 4, 32), jax.random.fold_in(own_keys[5], 1), 4, 31).astype(jnp.int32)
    receiver_depth = plant(jax.random.randint(own_keys[6], (NX, NY), 0, NZ // 4), jax.random.fold_in(own_keys[6], 1), 0, (NZ // 4) - 1).astype(jnp.int32)
    receiver_field = gaussian(own_keys[7], (NZ, NX, NY), 1.0, 6.0, ((1, 32), (2, 2)), jnp.float32)
    return dict(pressure=pressure, pressure_prior=pressure_prior, courant_square=courant_square, wavelet=wavelet, delay_steps=delay_steps, source_depth=source_depth, receiver_depth=receiver_depth, receiver_field=receiver_field)


CENTER = -205.0 / 72.0
COEFS = (1.6, -0.2, 8.0 / 315.0, -1.0 / 560.0)


def laplacian(field):
    depth, width, length = field.shape
    padded = jnp.pad(field, 4)
    total = (3.0 * CENTER) * field
    for k in range(1, 5):
        near = padded[4 + k:4 + k + depth, 4:4 + width, 4:4 + length] + padded[4 - k:4 - k + depth, 4:4 + width, 4:4 + length]
        near = near + padded[4:4 + depth, 4 + k:4 + k + width, 4:4 + length] + padded[4:4 + depth, 4 - k:4 - k + width, 4:4 + length]
        near = near + padded[4:4 + depth, 4:4 + width, 4 + k:4 + k + length] + padded[4:4 + depth, 4:4 + width, 4 - k:4 - k + length]
        total = total + COEFS[k - 1] * near
    return total


def injection(step, wavelet, delay_steps, source_depth, depth):
    picks = jnp.arange(wavelet.shape[0], dtype=jnp.int32)
    onehot = (picks[:, None, None] == (delay_steps + step)[None]).astype(wavelet.dtype)
    amplitude = jnp.sum(onehot * wavelet[:, None, None], axis=0)
    levels = jnp.arange(depth, dtype=jnp.int32)[:, None, None]
    return jnp.where(levels == source_depth[None], amplitude[None], jnp.zeros_like(amplitude)[None])


def reference(pressure, pressure_prior, courant_square, wavelet, delay_steps, source_depth, receiver_depth, receiver_field):
    depth = pressure.shape[0]
    coefficient = courant_square.astype(jnp.float32)
    current, prior = pressure, pressure_prior
    for step in range(STEPS):
        nxt = 2.0 * current - prior + coefficient * laplacian(current) + injection(step, wavelet, delay_steps, source_depth, depth)
        prior, current = current, nxt
    levels = jnp.arange(depth, dtype=jnp.int32)[:, None, None]
    masked = jnp.where(levels >= receiver_depth[None], receiver_field, jnp.zeros_like(receiver_field))
    product = current * masked
    padded = jnp.pad(product, ((1, 1), (0, 0), (0, 0)))
    image = 2.0 * product - padded[:-2] - padded[2:]
    return current, image
```

```python
import functools

import jax
import jax.numpy as jnp
from jax import lax
from jax.experimental import pallas as pl
from jax.experimental.pallas import tpu as pltpu
from jax.sharding import PartitionSpec as P

STEPS = 8

CENTER = -205.0 / 72.0
COEFS = (1.6, -0.2, 8.0 / 315.0, -1.0 / 560.0)
REACH = len(COEFS)
CHUNK = 32

VM = pl.BlockSpec(memory_space=pltpu.VMEM)
SM = pl.BlockSpec(memory_space=pltpu.SMEM)
F32 = jnp.float32


def split_planes(src_ref, odd, put):
    depth = src_ref.shape[0] // (2 * REACH)
    for i in range(REACH):
        right = src_ref[pl.ds(REACH + i, depth, stride=2 * REACH), :].T
        left = src_ref[pl.ds(REACH - 1 - i, depth, stride=2 * REACH), :].T
        put(i, jnp.where(odd, left, right), jnp.where(odd, right, left))


def rim(plane_ref, i, first):
    length = plane_ref.shape[1]
    return jnp.where(first, plane_ref[i, length - REACH : length, :], plane_ref[i, 0:REACH, :])


def open_kernel(flags_ref, p_ref, near_ref, far_ref, rim_ref):
    odd = flags_ref[0] == 1
    first = flags_ref[1] == 0

    def put(i, near, far):
        near_ref[i] = near
        far_ref[i] = far

    split_planes(p_ref, odd, put)
    for i in range(REACH):
        rim_ref[i] = rim(near_ref, i, first)
        rim_ref[REACH + i] = rim(far_ref, i, first)


def tables_kernel(
    flags_ref, wavelet_ref, prior_ref, coef_ref, delay_ref, depth_ref,
    prior_near, prior_far, coef_near, coef_far, mark_near, mark_far, amp_ref,
):
    odd = flags_ref[0] == 1
    length, depth = prior_near.shape[1:]

    def put_prior(i, near, far):
        prior_near[i] = near
        prior_far[i] = far

    def put_coef(i, near, far):
        coef_near[i] = near
        coef_far[i] = far

    split_planes(prior_ref, odd, put_prior)
    split_planes(coef_ref, odd, put_coef)
    delay = delay_ref[...]
    rows = []
    for step in range(STEPS):
        amplitude = jnp.zeros(delay.shape, F32)
        for w in range(wavelet_ref.shape[0]):
            amplitude = jnp.where(delay + step == w, wavelet_ref[w], amplitude)
        rows.append(amplitude)
    rows.append(depth_ref[...].astype(F32))
    fill = jnp.zeros((length - len(rows) * 2 * REACH, length), F32)
    columns = jnp.concatenate(rows + [fill], axis=0).T
    amp_ref[...] = columns
    levels = lax.broadcasted_iota(jnp.int32, (length, depth), 1).astype(F32)
    base = STEPS * 2 * REACH
    for i in range(REACH):
        right = columns[:, base + REACH + i : base + REACH + i + 1]
        left = columns[:, base + REACH - 1 - i : base + REACH - i]
        near = jnp.where(odd, left, right)
        far = jnp.where(odd, right, left)
        mark_near[i] = jnp.where(levels == near, 1.0, 0.0)
        mark_far[i] = jnp.where(levels == far, 1.0, 0.0)


def advance_kernel(
    step, half, flags_ref, self_ref, other_ref, halo_ref, rim_in_ref, prior_ref, coef_ref, mark_ref, amp_ref, *rest
):
    if half:
        near_new_ref, out_ref, rim_ref, pad_ref, deep_ref = rest
    else:
        out_ref, pad_ref, deep_ref = rest
    odd = flags_ref[0] == 1
    first = flags_ref[1] == 0
    planes, length, depth = self_ref.shape
    for i in range(planes):
        edge = rim_in_ref[half * REACH + i]
        none = jnp.zeros_like(edge)
        pad_ref[i, 8 : 8 + length, :] = self_ref[i]
        pad_ref[i, 8 - REACH : 8, :] = jnp.where(first, none, edge)
        pad_ref[i, 8 + length : 8 + length + REACH, :] = jnp.where(first, edge, none)
    apart = jnp.abs(
        lax.broadcasted_iota(jnp.int32, (depth, depth), 0) - lax.broadcasted_iota(jnp.int32, (depth, depth), 1)
    )
    band = jnp.where(apart == 0, F32(3.0 * CENTER), F32(0.0))
    for k in range(1, REACH + 1):
        band = jnp.where(apart == k, F32(COEFS[k - 1]), band)
    line = [(other_ref, REACH - 1 - i) for i in range(REACH)]
    line += [(self_ref, i) for i in range(REACH)]
    line += [(halo_ref, REACH - 1 - i) for i in range(REACH)]
    for i in range(planes):
        deep_ref[...] = jnp.dot(self_ref[i], band, precision=lax.Precision.HIGHEST, preferred_element_type=F32)
        right, left = REACH + i, REACH - 1 - i
        even_col, odd_col = (left, right) if half else (right, left)
        for row in range(0, length, CHUNK):
            at = slice(row, row + CHUNK)
            total = deep_ref[at, :]
            for k in range(1, REACH + 1):
                low_ref, low = line[REACH + i - k]
                high_ref, high = line[REACH + i + k]
                around = low_ref[low, at, :] + high_ref[high, at, :]
                around = around + pad_ref[i, 8 + row - k : 8 + row - k + CHUNK, :]
                around = around + pad_ref[i, 8 + row + k : 8 + row + k + CHUNK, :]
                total = total + COEFS[k - 1] * around
            column = step * 2 * REACH
            amplitude = jnp.where(
                odd,
                amp_ref[at, column + odd_col : column + odd_col + 1],
                amp_ref[at, column + even_col : column + even_col + 1],
            )
            out_ref[i, at, :] = (
                2.0 * self_ref[i, at, :]
                - prior_ref[i, at, :]
                + coef_ref[i, at, :] * total
                + mark_ref[i, at, :] * amplitude
            )
    if half:
        for i in range(planes):
            rim_ref[i] = rim(near_new_ref, i, first)
            rim_ref[REACH + i] = rim(out_ref, i, first)


def close_kernel(flags_ref, near_ref, far_ref, receiver_ref, receiver_depth_ref, p_ref, image_ref, product_ref):
    odd = flags_ref[0] == 1
    width = 2 * REACH
    depth = p_ref.shape[0] // width
    for i in range(REACH):
        near, far = near_ref[i], far_ref[i]
        p_ref[pl.ds(REACH + i, depth, stride=width), :] = jnp.where(odd, far, near).T
        p_ref[pl.ds(REACH - 1 - i, depth, stride=width), :] = jnp.where(odd, near, far).T
    start = receiver_depth_ref[...]
    for z in range(depth):
        at = slice(z * width, (z + 1) * width)
        field = receiver_ref[at, :]
        product_ref[at, :] = p_ref[at, :] * jnp.where(start <= z, field, jnp.zeros_like(field))
    for z in range(depth):
        at = slice(z * width, (z + 1) * width)
        value = 2.0 * product_ref[at, :]
        if z > 0:
            value = value - product_ref[(z - 1) * width : z * width, :]
        if z < depth - 1:
            value = value - product_ref[(z + 1) * width : (z + 2) * width, :]
        image_ref[at, :] = value


def pairs(size, first):
    left = [(i, i + 1) for i in range(first, size - 1, 2)]
    return left + [(b, a) for a, b in left]


def shards(
    pressure,
    pressure_prior,
    courant_square,
    wavelet,
    delay_steps,
    source_depth,
    receiver_depth,
    receiver_field,
):
    depth, width, length = pressure.shape
    size = lax.axis_size("gx")
    even, uneven = pairs(size, 0), pairs(size, 1)
    swap = pairs(lax.axis_size("gy"), 0)
    flags = jnp.stack([lax.axis_index("gx") % 2, lax.axis_index("gy")]).astype(jnp.int32)
    flat = (depth * width, length)
    half = jax.ShapeDtypeStruct((REACH, length, depth), F32)
    rims = jax.ShapeDtypeStruct((2 * REACH, REACH, depth), F32)
    square = jax.ShapeDtypeStruct((length, length), F32)

    near, far, edge = pl.pallas_call(
        open_kernel, out_shape=(half, half, rims), in_specs=[SM, VM], out_specs=(VM, VM, VM), name="open"
    )(flags, pressure.reshape(flat))
    near_prior, far_prior, near_coef, far_coef, near_mark, far_mark, amp = pl.pallas_call(
        tables_kernel,
        out_shape=(half,) * 6 + (square,),
        in_specs=[SM, SM] + [VM] * 4,
        out_specs=(VM,) * 7,
        name="tables",
    )(
        flags,
        wavelet,
        pressure_prior.reshape(flat),
        courant_square.astype(F32).reshape(flat),
        delay_steps,
        source_depth,
    )
    scratch = [pltpu.VMEM((REACH, length + 16, depth), F32), pltpu.VMEM((length, depth), F32)]
    for step in range(STEPS):
        near_halo = lax.ppermute(near, "gx", even)
        far_halo = lax.ppermute(far, "gx", uneven)
        edge_in = lax.ppermute(edge, "gy", swap)
        near_next = pl.pallas_call(
            functools.partial(advance_kernel, step, 0),
            out_shape=half,
            in_specs=[SM] + [VM] * 8,
            out_specs=VM,
            scratch_shapes=scratch,
            name=f"near{step}",
        )(flags, near, far, near_halo, edge_in, near_prior, near_coef, near_mark, amp)
        far_next, edge = pl.pallas_call(
            functools.partial(advance_kernel, step, 1),
            out_shape=(half, rims),
            in_specs=[SM] + [VM] * 9,
            out_specs=(VM, VM),
            scratch_shapes=scratch,
            name=f"far{step}",
        )(flags, far, near, far_halo, edge_in, far_prior, far_coef, far_mark, amp, near_next)
        near_prior, far_prior = near, far
        near, far = near_next, far_next
    final, filtered = pl.pallas_call(
        close_kernel,
        out_shape=(jax.ShapeDtypeStruct(flat, F32), jax.ShapeDtypeStruct(flat, F32)),
        in_specs=[SM] + [VM] * 4,
        out_specs=(VM, VM),
        scratch_shapes=[pltpu.VMEM(flat, F32)],
        name="close",
    )(flags, near, far, receiver_field.reshape(flat), receiver_depth)
    image = lax.all_to_all(filtered.reshape(depth, width, length), "gx", split_axis=0, concat_axis=1, tiled=True)
    return final.reshape(depth, width, length), image


def solution(mesh):
    in_specs = (
        P(None, ("shots", "gx"), "gy"),
        P(None, ("shots", "gx"), "gy"),
        P(None, "gx", "gy"),
        P("shots"),
        P(("shots", "gx"), "gy"),
        P(("shots", "gx"), "gy"),
        P(("shots", "gx"), "gy"),
        P(None, ("shots", "gx"), "gy"),
    )
    out_specs = (P(None, ("shots", "gx"), "gy"), P("gx", "shots", "gy"))
    return jax.shard_map(shards, mesh=mesh, in_specs=in_specs, out_specs=out_specs, check_vma=False)
```

```python
import functools

import jax
import jax.numpy as jnp
from jax import lax
from jax.experimental import pallas as pl
from jax.experimental.pallas import tpu as pltpu
from jax.sharding import PartitionSpec as P

STEPS = 8

CENTER = -205.0 / 72.0
COEFS = (1.6, -0.2, 8.0 / 315.0, -1.0 / 560.0)
REACH = len(COEFS)
CHUNK = 32

VM = pl.BlockSpec(memory_space=pltpu.VMEM)
SM = pl.BlockSpec(memory_space=pltpu.SMEM)
F32 = jnp.float32
PARAMS = pltpu.CompilerParams(vmem_limit_bytes=8 * 2**20)


def split_planes(src_ref, odd, put):
    depth = src_ref.shape[0] // (2 * REACH)
    for i in range(REACH):
        right = src_ref[pl.ds(REACH + i, depth, stride=2 * REACH), :].T
        left = src_ref[pl.ds(REACH - 1 - i, depth, stride=2 * REACH), :].T
        put(i, jnp.where(odd, left, right), jnp.where(odd, right, left))


def rim(plane_ref, i, first):
    length = plane_ref.shape[1]
    return jnp.where(first, plane_ref[i, length - REACH : length, :], plane_ref[i, 0:REACH, :])


def open_kernel(flags_ref, p_ref, near_ref, far_ref, rim_ref):
    odd = flags_ref[0] == 1
    first = flags_ref[1] == 0

    def put(i, near, far):
        near_ref[i] = near
        far_ref[i] = far

    split_planes(p_ref, odd, put)
    for i in range(REACH):
        rim_ref[i] = rim(near_ref, i, first)
        rim_ref[REACH + i] = rim(far_ref, i, first)


def tables_kernel(
    flags_ref, wavelet_ref, prior_ref, coef_ref, delay_ref, depth_ref,
    prior_near, prior_far, coef_near, coef_far, mark_near, mark_far, amp_ref,
):
    odd = flags_ref[0] == 1
    length, depth = prior_near.shape[1:]

    def put_prior(i, near, far):
        prior_near[i] = near
        prior_far[i] = far

    def put_coef(i, near, far):
        coef_near[i] = near
        coef_far[i] = far

    split_planes(prior_ref, odd, put_prior)
    split_planes(coef_ref, odd, put_coef)
    delay = delay_ref[...]
    rows = []
    for step in range(STEPS):
        amplitude = jnp.zeros(delay.shape, F32)
        for w in range(wavelet_ref.shape[0]):
            amplitude = jnp.where(delay + step == w, wavelet_ref[w], amplitude)
        rows.append(amplitude)
    rows.append(depth_ref[...].astype(F32))
    fill = jnp.zeros((length - len(rows) * 2 * REACH, length), F32)
    columns = jnp.concatenate(rows + [fill], axis=0).T
    amp_ref[...] = columns
    levels = lax.broadcasted_iota(jnp.int32, (length, depth), 1).astype(F32)
    base = STEPS * 2 * REACH
    for i in range(REACH):
        right = columns[:, base + REACH + i : base + REACH + i + 1]
        left = columns[:, base + REACH - 1 - i : base + REACH - i]
        near = jnp.where(odd, left, right)
        far = jnp.where(odd, right, left)
        mark_near[i] = jnp.where(levels == near, 1.0, 0.0)
        mark_far[i] = jnp.where(levels == far, 1.0, 0.0)


def advance_kernel(
    step, half, flags_ref, self_ref, other_ref, halo_ref, rim_in_ref, prior_ref, coef_ref, mark_ref, amp_ref, *rest
):
    if half:
        near_new_ref, out_ref, rim_ref, pad_ref, deep_ref = rest
    else:
        out_ref, pad_ref, deep_ref = rest
    odd = flags_ref[0] == 1
    first = flags_ref[1] == 0
    planes, length, depth = self_ref.shape
    for i in range(planes):
        edge = rim_in_ref[half * REACH + i]
        none = jnp.zeros_like(edge)
        pad_ref[i, 8 : 8 + length, :] = self_ref[i]
        pad_ref[i, 8 - REACH : 8, :] = jnp.where(first, none, edge)
        pad_ref[i, 8 + length : 8 + length + REACH, :] = jnp.where(first, edge, none)
    apart = jnp.abs(
        lax.broadcasted_iota(jnp.int32, (depth, depth), 0) - lax.broadcasted_iota(jnp.int32, (depth, depth), 1)
    )
    band = jnp.where(apart == 0, F32(3.0 * CENTER), F32(0.0))
    for k in range(1, REACH + 1):
        band = jnp.where(apart == k, F32(COEFS[k - 1]), band)
    line = [(other_ref, REACH - 1 - i) for i in range(REACH)]
    line += [(self_ref, i) for i in range(REACH)]
    line += [(halo_ref, REACH - 1 - i) for i in range(REACH)]
    for i in range(planes):
        deep_ref[...] = jnp.dot(self_ref[i], band, precision=lax.Precision.HIGHEST, preferred_element_type=F32)
        right, left = REACH + i, REACH - 1 - i
        even_col, odd_col = (left, right) if half else (right, left)
        for row in range(0, length, CHUNK):
            at = slice(row, row + CHUNK)
            total = deep_ref[at, :]
            for k in range(1, REACH + 1):
                low_ref, low = line[REACH + i - k]
                high_ref, high = line[REACH + i + k]
                around = low_ref[low, at, :] + high_ref[high, at, :]
                around = around + pad_ref[i, 8 + row - k : 8 + row - k + CHUNK, :]
                around = around + pad_ref[i, 8 + row + k : 8 + row + k + CHUNK, :]
                total = total + COEFS[k - 1] * around
            column = step * 2 * REACH
            amplitude = jnp.where(
                odd,
                amp_ref[at, column + odd_col : column + odd_col + 1],
                amp_ref[at, column + even_col : column + even_col + 1],
            )
            out_ref[i, at, :] = (
                2.0 * self_ref[i, at, :]
                - prior_ref[i, at, :]
                + coef_ref[i, at, :] * total
                + mark_ref[i, at, :] * amplitude
            )
    if half:
        for i in range(planes):
            rim_ref[i] = rim(near_new_ref, i, first)
            rim_ref[REACH + i] = rim(out_ref, i, first)


def close_kernel(flags_ref, near_ref, far_ref, receiver_ref, receiver_depth_ref, p_ref, image_ref, product_ref):
    odd = flags_ref[0] == 1
    width = 2 * REACH
    depth = p_ref.shape[0] // width
    for i in range(REACH):
        near, far = near_ref[i], far_ref[i]
        p_ref[pl.ds(REACH + i, depth, stride=width), :] = jnp.where(odd, far, near).T
        p_ref[pl.ds(REACH - 1 - i, depth, stride=width), :] = jnp.where(odd, near, far).T
    start = receiver_depth_ref[...]
    for z in range(depth):
        at = slice(z * width, (z + 1) * width)
        field = receiver_ref[at, :]
        product_ref[at, :] = p_ref[at, :] * jnp.where(start <= z, field, jnp.zeros_like(field))
    for z in range(depth):
        at = slice(z * width, (z + 1) * width)
        value = 2.0 * product_ref[at, :]
        if z > 0:
            value = value - product_ref[(z - 1) * width : z * width, :]
        if z < depth - 1:
            value = value - product_ref[(z + 1) * width : (z + 2) * width, :]
        image_ref[at, :] = value


def pairs(size, first):
    left = [(i, i + 1) for i in range(first, size - 1, 2)]
    return left + [(b, a) for a, b in left]


def shards(
    pressure,
    pressure_prior,
    courant_square,
    wavelet,
    delay_steps,
    source_depth,
    receiver_depth,
    receiver_field,
):
    depth, width, length = pressure.shape
    size = lax.axis_size("gx")
    even, uneven = pairs(size, 0), pairs(size, 1)
    swap = pairs(lax.axis_size("gy"), 0)
    flags = jnp.stack([lax.axis_index("gx") % 2, lax.axis_index("gy")]).astype(jnp.int32)
    flat = (depth * width, length)
    half = jax.ShapeDtypeStruct((REACH, length, depth), F32)
    rims = jax.ShapeDtypeStruct((2 * REACH, REACH, depth), F32)
    square = jax.ShapeDtypeStruct((length, length), F32)

    near, far, edge = pl.pallas_call(
        open_kernel, out_shape=(half, half, rims), in_specs=[SM, VM], out_specs=(VM, VM, VM), compiler_params=PARAMS, name="open"
    )(flags, pressure.reshape(flat))
    near_prior, far_prior, near_coef, far_coef, near_mark, far_mark, amp = pl.pallas_call(
        tables_kernel,
        out_shape=(half,) * 6 + (square,),
        in_specs=[SM, SM] + [VM] * 4,
        out_specs=(VM,) * 7,
        compiler_params=PARAMS, name="tables",
    )(
        flags,
        wavelet,
        pressure_prior.reshape(flat),
        courant_square.astype(F32).reshape(flat),
        delay_steps,
        source_depth,
    )
    scratch = [pltpu.VMEM((REACH, length + 16, depth), F32), pltpu.VMEM((length, depth), F32)]
    for step in range(STEPS):
        near_halo = lax.ppermute(near, "gx", even)
        far_halo = lax.ppermute(far, "gx", uneven)
        edge_in = lax.ppermute(edge, "gy", swap)
        near_next = pl.pallas_call(
            functools.partial(advance_kernel, step, 0),
            out_shape=half,
            in_specs=[SM] + [VM] * 8,
            out_specs=VM,
            scratch_shapes=scratch,
            compiler_params=PARAMS, name=f"near{step}",
        )(flags, near, far, near_halo, edge_in, near_prior, near_coef, near_mark, amp)
        far_next, edge = pl.pallas_call(
            functools.partial(advance_kernel, step, 1),
            out_shape=(half, rims),
            in_specs=[SM] + [VM] * 9,
            out_specs=(VM, VM),
            scratch_shapes=scratch,
            compiler_params=PARAMS, name=f"far{step}",
        )(flags, far, near, far_halo, edge_in, far_prior, far_coef, far_mark, amp, near_next)
        near_prior, far_prior = near, far
        near, far = near_next, far_next
    final, filtered = pl.pallas_call(
        close_kernel,
        out_shape=(jax.ShapeDtypeStruct(flat, F32), jax.ShapeDtypeStruct(flat, F32)),
        in_specs=[SM] + [VM] * 4,
        out_specs=(VM, VM),
        scratch_shapes=[pltpu.VMEM(flat, F32)],
        compiler_params=PARAMS, name="close",
    )(flags, near, far, receiver_field.reshape(flat), receiver_depth)
    image = lax.all_to_all(filtered.reshape(depth, width, length), "gx", split_axis=0, concat_axis=1, tiled=True)
    return final.reshape(depth, width, length), image


def solution(mesh):
    in_specs = (
        P(None, ("shots", "gx"), "gy"),
        P(None, ("shots", "gx"), "gy"),
        P(None, "gx", "gy"),
        P("shots"),
        P(("shots", "gx"), "gy"),
        P(("shots", "gx"), "gy"),
        P(("shots", "gx"), "gy"),
        P(None, ("shots", "gx"), "gy"),
    )
    out_specs = (P(None, ("shots", "gx"), "gy"), P("gx", "shots", "gy"))
    return jax.shard_map(shards, mesh=mesh, in_specs=in_specs, out_specs=out_specs, check_vma=False)
```

```python
import functools

import jax
import jax.numpy as jnp
from jax import lax
from jax.experimental import pallas as pl
from jax.experimental.pallas import tpu as pltpu
from jax.sharding import PartitionSpec as P

STEPS = 8

CENTER = -205.0 / 72.0
COEFS = (1.6, -0.2, 8.0 / 315.0, -1.0 / 560.0)
REACH = len(COEFS)
CHUNK = 32

VM = pl.BlockSpec(memory_space=pltpu.VMEM)
F32 = jnp.float32
BF16 = jnp.bfloat16
PARAMS = pltpu.CompilerParams(vmem_limit_bytes=8 * 2**20)


def choose(flag, shape, yes, no):
    return jnp.where(jnp.broadcast_to(flag, shape) > 0.5, yes, no)


def split_planes(src_ref, odd, put):
    depth = src_ref.shape[0] // (2 * REACH)
    for i in range(REACH):
        right = src_ref[pl.ds(REACH + i, depth, stride=2 * REACH), :].T
        left = src_ref[pl.ds(REACH - 1 - i, depth, stride=2 * REACH), :].T
        put(i, choose(odd, right.shape, left, right), choose(odd, right.shape, right, left))


def rim(plane_ref, i, first):
    length, depth = plane_ref.shape[1:]
    return choose(first, (REACH, depth), plane_ref[i, length - REACH : length, :], plane_ref[i, 0:REACH, :])


def open_kernel(sides_ref, p_ref, near_ref, far_ref, rim_ref):
    odd = sides_ref[0:1, :]
    first = sides_ref[1:2, :]

    def put(i, near, far):
        near_ref[i] = near
        far_ref[i] = far

    split_planes(p_ref, odd, put)
    for i in range(REACH):
        rim_ref[i] = rim(near_ref, i, first)
        rim_ref[REACH + i] = rim(far_ref, i, first)


def tables_kernel(
    sides_ref, wavelet_ref, prior_ref, coef_ref, delay_ref, depth_ref,
    prior_near, prior_far, coef_near, coef_far, mark_near, mark_far, amp_ref,
):
    odd = sides_ref[0:1, :]
    length, depth = prior_near.shape[1:]

    def put_prior(i, near, far):
        prior_near[i] = near
        prior_far[i] = far

    def put_coef(i, near, far):
        coef_near[i] = near
        coef_far[i] = far

    split_planes(prior_ref, odd, put_prior)
    split_planes(coef_ref, odd, put_coef)

    def arrange(rows):
        right = [rows[REACH + i : REACH + i + 1, :] for i in range(REACH)]
        left = [rows[REACH - 1 - i : REACH - i, :] for i in range(REACH)]
        return choose(odd, rows.shape, jnp.concatenate(left + right, axis=0), jnp.concatenate(right + left, axis=0))

    delay = delay_ref[...]
    rows = []
    for step in range(STEPS):
        amplitude = jnp.zeros(delay.shape, F32)
        for w in range(wavelet_ref.shape[0]):
            wave = jnp.broadcast_to(wavelet_ref[w : w + 1, :], delay.shape)
            amplitude = jnp.where(delay + step == w, wave, amplitude)
        rows.append(arrange(amplitude))
    rows.append(arrange(depth_ref[...].astype(F32)))
    fill = jnp.zeros((length - len(rows) * 2 * REACH, length), F32)
    columns = jnp.concatenate(rows + [fill], axis=0).T
    amp_ref[...] = columns
    levels = lax.broadcasted_iota(jnp.int32, (length, depth), 1).astype(F32)
    base = STEPS * 2 * REACH
    for i in range(REACH):
        mark_near[i] = jnp.where(levels == columns[:, base + i : base + i + 1], 1.0, 0.0)
        mark_far[i] = jnp.where(levels == columns[:, base + REACH + i : base + REACH + i + 1], 1.0, 0.0)


def advance_kernel(
    step, half, sides_ref, self_ref, other_ref, halo_ref, rim_in_ref, prior_ref, coef_ref, mark_ref, amp_ref, *rest
):
    pad_ref, deep_ref = rest[-2:]
    first = sides_ref[1:2, :]
    planes, length, depth = self_ref.shape
    if half:
        near_new_ref, out_ref, rim_ref = rest[:3]
    else:
        out_ref = rest[0]
    for i in range(planes):
        edge = rim_in_ref[half * REACH + i]
        none = jnp.zeros_like(edge)
        pad_ref[i, 8 : 8 + length, :] = self_ref[i]
        pad_ref[i, 8 - REACH : 8, :] = choose(first, edge.shape, none, edge)
        pad_ref[i, 8 + length : 8 + length + REACH, :] = choose(first, edge.shape, edge, none)
    apart = jnp.abs(
        lax.broadcasted_iota(jnp.int32, (depth, depth), 0) - lax.broadcasted_iota(jnp.int32, (depth, depth), 1)
    )
    band = jnp.where(apart == 0, F32(3.0 * CENTER), F32(0.0))
    for k in range(1, REACH + 1):
        band = jnp.where(apart == k, F32(COEFS[k - 1]), band)
    band_high = band.astype(BF16)
    band_low = (band - band_high.astype(F32)).astype(BF16)
    flat = self_ref[...].reshape(planes * length, depth)
    high = flat.astype(BF16)
    low = (flat - high.astype(F32)).astype(BF16)
    dot = functools.partial(jnp.dot, preferred_element_type=F32)
    deep_ref[...] = dot(high, band_high) + (dot(low, band_high) + dot(high, band_low))
    for row in range(0, length, CHUNK):
        at = slice(row, row + CHUNK)
        line = [other_ref[REACH - 1 - i, at, :] for i in range(REACH)]
        line += [self_ref[i, at, :] for i in range(REACH)]
        line += [halo_ref[REACH - 1 - i, at, :] for i in range(REACH)]
        for i in range(planes):
            total = deep_ref[i * length + row : i * length + row + CHUNK, :]
            for k in range(1, REACH + 1):
                around = line[REACH + i - k] + line[REACH + i + k]
                around = around + pad_ref[i, 8 + row - k : 8 + row - k + CHUNK, :]
                around = around + pad_ref[i, 8 + row + k : 8 + row + k + CHUNK, :]
                total = total + COEFS[k - 1] * around
            column = (step * 2 + half) * REACH + i
            out_ref[i, at, :] = (
                2.0 * line[REACH + i]
                - prior_ref[i, at, :]
                + coef_ref[i, at, :] * total
                + mark_ref[i, at, :] * amp_ref[at, column : column + 1]
            )
    if half:
        for i in range(planes):
            rim_ref[i] = rim(near_new_ref, i, first)
            rim_ref[REACH + i] = rim(out_ref, i, first)


def close_kernel(sides_ref, near_ref, far_ref, receiver_ref, receiver_depth_ref, p_ref, image_ref, product_ref):
    odd = sides_ref[0:1, :]
    width = 2 * REACH
    depth = p_ref.shape[0] // width
    for i in range(REACH):
        near, far = near_ref[i], far_ref[i]
        p_ref[pl.ds(REACH + i, depth, stride=width), :] = choose(odd, near.shape, far, near).T
        p_ref[pl.ds(REACH - 1 - i, depth, stride=width), :] = choose(odd, near.shape, near, far).T
    start = receiver_depth_ref[...]
    for z in range(depth):
        at = slice(z * width, (z + 1) * width)
        field = receiver_ref[at, :]
        product_ref[at, :] = p_ref[at, :] * jnp.where(start <= z, field, jnp.zeros_like(field))
    for z in range(depth):
        at = slice(z * width, (z + 1) * width)
        value = 2.0 * product_ref[at, :]
        if z > 0:
            value = value - product_ref[(z - 1) * width : z * width, :]
        if z < depth - 1:
            value = value - product_ref[(z + 1) * width : (z + 2) * width, :]
        image_ref[at, :] = value


def pairs(size, first):
    left = [(i, i + 1) for i in range(first, size - 1, 2)]
    return left + [(b, a) for a, b in left]


def shards(
    pressure,
    pressure_prior,
    courant_square,
    wavelet,
    delay_steps,
    source_depth,
    receiver_depth,
    receiver_field,
):
    depth, width, length = pressure.shape
    size, cores = lax.axis_size("gx"), lax.axis_size("gy")
    near_pairs, far_pairs = pairs(size, 0), pairs(size, 1)
    rim_pairs = pairs(cores, 0)
    odd = lax.axis_index("gx") % 2
    first = jnp.where(lax.axis_index("gy") == 0, 1, 0)
    rows = lax.broadcasted_iota(jnp.int32, (8, length), 0)
    sides = jnp.where(rows == 0, odd, first).astype(F32)
    flat = (depth * width, length)
    half = jax.ShapeDtypeStruct((REACH, length, depth), F32)
    rims = jax.ShapeDtypeStruct((2 * REACH, REACH, depth), F32)
    square = jax.ShapeDtypeStruct((length, length), F32)
    wave = jnp.broadcast_to(wavelet[:, None], (wavelet.shape[0], length))

    def kernel(body, outs, inputs, scratch=(), name=None):
        return pl.pallas_call(
            body,
            out_shape=outs,
            in_specs=[VM] * len(inputs),
            out_specs=jax.tree.map(lambda _: VM, outs),
            scratch_shapes=list(scratch),
            compiler_params=PARAMS,
            name=name,
        )(*inputs)

    near, far, edge = kernel(open_kernel, (half, half, rims), (sides, pressure.reshape(flat)), name="open")
    near_prior, far_prior, near_coef, far_coef, near_mark, far_mark, amp = kernel(
        tables_kernel,
        (half,) * 6 + (square,),
        (
            sides,
            wave,
            pressure_prior.reshape(flat),
            courant_square.astype(F32).reshape(flat),
            delay_steps,
            source_depth,
        ),
        name="tables",
    )
    scratch = (pltpu.VMEM((REACH, length + 16, depth), F32), pltpu.VMEM((REACH * length, depth), F32))
    for step in range(STEPS):
        near_halo = lax.ppermute(near, "gx", near_pairs)
        far_halo = lax.ppermute(far, "gx", far_pairs)
        edge_in = lax.ppermute(edge, "gy", rim_pairs)
        near_next = kernel(
            functools.partial(advance_kernel, step, 0),
            half,
            (sides, near, far, near_halo, edge_in, near_prior, near_coef, near_mark, amp),
            scratch,
            f"near{step}",
        )
        far_next, edge = kernel(
            functools.partial(advance_kernel, step, 1),
            (half, rims),
            (sides, far, near, far_halo, edge_in, far_prior, far_coef, far_mark, amp, near_next),
            scratch,
            f"far{step}",
        )
        near_prior, far_prior = near, far
        near, far = near_next, far_next
    whole = jax.ShapeDtypeStruct(flat, F32)
    final, filtered = kernel(
        close_kernel,
        (whole, whole),
        (sides, near, far, receiver_field.reshape(flat), receiver_depth),
        (pltpu.VMEM(flat, F32),),
        "close",
    )
    image = lax.all_to_all(filtered.reshape(depth, width, length), "gx", split_axis=0, concat_axis=1, tiled=True)
    return final.reshape(depth, width, length), image


def solution(mesh):
    in_specs = (
        P(None, ("shots", "gx"), "gy"),
        P(None, ("shots", "gx"), "gy"),
        P(None, "gx", "gy"),
        P("shots"),
        P(("shots", "gx"), "gy"),
        P(("shots", "gx"), "gy"),
        P(("shots", "gx"), "gy"),
        P(None, ("shots", "gx"), "gy"),
    )
    out_specs = (P(None, ("shots", "gx"), "gy"), P("gx", "shots", "gy"))
    return jax.shard_map(shards, mesh=mesh, in_specs=in_specs, out_specs=out_specs, check_vma=False)
```

```python
import functools

import jax
import jax.numpy as jnp
from jax import lax
from jax.experimental import pallas as pl
from jax.experimental.pallas import tpu as pltpu
from jax.sharding import PartitionSpec as P

STEPS = 8

CENTER = -205.0 / 72.0
COEFS = (1.6, -0.2, 8.0 / 315.0, -1.0 / 560.0)
REACH = len(COEFS)
CHUNK = 32

VM = pl.BlockSpec(memory_space=pltpu.VMEM)
F32 = jnp.float32
BF16 = jnp.bfloat16
PARAMS = pltpu.CompilerParams(vmem_limit_bytes=8 * 2**20)


def choose(flag, shape, yes, no):
    return jnp.where(jnp.broadcast_to(flag, shape) > 0.5, yes, no)


def split_planes(src_ref, odd, put):
    depth = src_ref.shape[0] // (2 * REACH)
    for i in range(REACH):
        right = src_ref[pl.ds(REACH + i, depth, stride=2 * REACH), :]
        left = src_ref[pl.ds(REACH - 1 - i, depth, stride=2 * REACH), :]
        put(i, choose(odd, right.shape, left, right).T, choose(odd, right.shape, right, left).T)


def rim(plane_ref, i, first):
    length, depth = plane_ref.shape[1:]
    return choose(first, (REACH, depth), plane_ref[i, length - REACH : length, :], plane_ref[i, 0:REACH, :])


def open_near_kernel(sides_ref, p_ref, near_ref):
    def put(i, near, far):
        near_ref[i] = near

    split_planes(p_ref, sides_ref[0:1, :], put)


def open_far_kernel(sides_ref, p_ref, near_ref, far_ref, rim_ref):
    first = sides_ref[1:2, :]

    def put(i, near, far):
        far_ref[i] = far

    split_planes(p_ref, sides_ref[0:1, :], put)
    for i in range(REACH):
        rim_ref[i] = rim(near_ref, i, first)
        rim_ref[REACH + i] = rim(far_ref, i, first)


def tables_kernel(
    sides_ref, wavelet_ref, prior_ref, coef_ref, delay_ref, depth_ref,
    prior_near, prior_far, coef_near, coef_far, mark_near, mark_far, amp_ref,
):
    odd = sides_ref[0:1, :]
    length, depth = prior_near.shape[1:]

    def put_prior(i, near, far):
        prior_near[i] = near
        prior_far[i] = far

    def put_coef(i, near, far):
        coef_near[i] = near
        coef_far[i] = far

    split_planes(prior_ref, odd, put_prior)
    split_planes(coef_ref, odd, put_coef)

    def arrange(rows):
        right = [rows[REACH + i : REACH + i + 1, :] for i in range(REACH)]
        left = [rows[REACH - 1 - i : REACH - i, :] for i in range(REACH)]
        return choose(odd, rows.shape, jnp.concatenate(left + right, axis=0), jnp.concatenate(right + left, axis=0))

    delay = delay_ref[...]
    rows = []
    for step in range(STEPS):
        amplitude = jnp.zeros(delay.shape, F32)
        for w in range(wavelet_ref.shape[0]):
            wave = jnp.broadcast_to(wavelet_ref[w : w + 1, :], delay.shape)
            amplitude = jnp.where(delay + step == w, wave, amplitude)
        rows.append(arrange(amplitude))
    rows.append(arrange(depth_ref[...].astype(F32)))
    fill = jnp.zeros((length - len(rows) * 2 * REACH, length), F32)
    columns = jnp.concatenate(rows + [fill], axis=0).T
    amp_ref[...] = columns
    levels = lax.broadcasted_iota(jnp.int32, (length, depth), 1).astype(F32)
    base = STEPS * 2 * REACH
    for i in range(REACH):
        mark_near[i] = jnp.where(levels == columns[:, base + i : base + i + 1], 1.0, 0.0)
        mark_far[i] = jnp.where(levels == columns[:, base + REACH + i : base + REACH + i + 1], 1.0, 0.0)


def advance_kernel(
    step, half, sides_ref, self_ref, other_ref, halo_ref, rim_in_ref, prior_ref, coef_ref, mark_ref, amp_ref, *rest
):
    pad_ref, deep_ref = rest[-2:]
    first = sides_ref[1:2, :]
    planes, length, depth = self_ref.shape
    if len(rest) > 3:
        near_new_ref, out_ref, rim_ref = rest[:3]
    else:
        out_ref, rim_ref = rest[0], None
    for i in range(planes):
        edge = rim_in_ref[half * REACH + i]
        none = jnp.zeros_like(edge)
        pad_ref[i, 8 : 8 + length, :] = self_ref[i]
        pad_ref[i, 8 - REACH : 8, :] = choose(first, edge.shape, none, edge)
        pad_ref[i, 8 + length : 8 + length + REACH, :] = choose(first, edge.shape, edge, none)
    apart = jnp.abs(
        lax.broadcasted_iota(jnp.int32, (depth, depth), 0) - lax.broadcasted_iota(jnp.int32, (depth, depth), 1)
    )
    band = jnp.where(apart == 0, F32(3.0 * CENTER), F32(0.0))
    for k in range(1, REACH + 1):
        band = jnp.where(apart == k, F32(COEFS[k - 1]), band)
    band_high = band.astype(BF16)
    band_low = (band - band_high.astype(F32)).astype(BF16)
    flat = self_ref[...].reshape(planes * length, depth)
    high = flat.astype(BF16)
    low = (flat - high.astype(F32)).astype(BF16)
    dot = functools.partial(jnp.dot, preferred_element_type=F32)
    deep_ref[...] = dot(high, band_high) + (dot(low, band_high) + dot(high, band_low))
    for row in range(0, length, CHUNK):
        at = slice(row, row + CHUNK)
        line = [other_ref[REACH - 1 - i, at, :] for i in range(REACH)]
        line += [self_ref[i, at, :] for i in range(REACH)]
        line += [halo_ref[REACH - 1 - i, at, :] for i in range(REACH)]
        for i in range(planes):
            total = deep_ref[i * length + row : i * length + row + CHUNK, :]
            for k in range(1, REACH + 1):
                around = line[REACH + i - k] + line[REACH + i + k]
                around = around + pad_ref[i, 8 + row - k : 8 + row - k + CHUNK, :]
                around = around + pad_ref[i, 8 + row + k : 8 + row + k + CHUNK, :]
                total = total + COEFS[k - 1] * around
            column = (step * 2 + half) * REACH + i
            out_ref[i, at, :] = (
                2.0 * line[REACH + i]
                - prior_ref[i, at, :]
                + coef_ref[i, at, :] * total
                + mark_ref[i, at, :] * amp_ref[at, column : column + 1]
            )
    if rim_ref is not None:
        for i in range(planes):
            rim_ref[i] = rim(near_new_ref, i, first)
            rim_ref[REACH + i] = rim(out_ref, i, first)


def image_half(is_near, sides_ref, half_ref, receiver_ref, receiver_depth_ref, image_ref, pad_ref, row, stride):
    odd = sides_ref[0:1, :]
    length, depth = half_ref.shape[1:]
    width = 2 * REACH
    levels = lax.broadcasted_iota(jnp.int32, (depth, length), 0).astype(F32)
    start = receiver_depth_ref[...].astype(F32)
    pad_ref[0:8, :] = jnp.zeros((8, length), F32)
    pad_ref[8 + depth : 16 + depth, :] = jnp.zeros((8, length), F32)
    for j in range(REACH):
        rising, falling = half_ref[j], half_ref[REACH - 1 - j]
        low = receiver_ref[pl.ds(j, depth, stride=width), :]
        high = receiver_ref[pl.ds(REACH + j, depth, stride=width), :]
        start_low, start_high = start[j : j + 1, :], start[REACH + j : REACH + j + 1, :]
        if is_near:
            field = choose(odd, rising.shape, falling, rising).T
            receiver = choose(odd, low.shape, low, high)
            begin = choose(odd, start_low.shape, start_low, start_high)
        else:
            field = choose(odd, rising.shape, rising, falling).T
            receiver = choose(odd, low.shape, high, low)
            begin = choose(odd, start_low.shape, start_high, start_low)
        begin = jnp.broadcast_to(begin, levels.shape)
        product = field * jnp.where(levels >= begin, receiver, jnp.zeros_like(receiver))
        pad_ref[8 : 8 + depth, :] = product
        image_ref[pl.ds(row + j, depth, stride=stride), :] = (
            2.0 * product - pad_ref[7 : 7 + depth, :] - pad_ref[9 : 9 + depth, :]
        )


def image_near_kernel(sides_ref, near_ref, receiver_ref, receiver_depth_ref, image_ref, pad_ref):
    image_half(True, sides_ref, near_ref, receiver_ref, receiver_depth_ref, image_ref, pad_ref, 0, REACH)


def last_kernel(step, sides_ref, *rest):
    receiver_ref, receiver_depth_ref, part_ref, far_ref, image_ref, side_ref, deep_ref, pad_ref = rest[-8:]
    advance_kernel(step, 1, sides_ref, *rest[:-8], far_ref, side_ref, deep_ref)
    width = 2 * REACH
    depth = part_ref.shape[0] // REACH
    image_half(False, sides_ref, far_ref, receiver_ref, receiver_depth_ref, image_ref, pad_ref, REACH, width)
    for j in range(REACH):
        image_ref[pl.ds(j, depth, stride=width), :] = part_ref[pl.ds(j, depth, stride=REACH), :]


def final_kernel(sides_ref, near_ref, far_ref, p_ref):
    odd = sides_ref[0:1, :]
    width = 2 * REACH
    depth = p_ref.shape[0] // width
    for i in range(REACH):
        near, far = near_ref[i], far_ref[i]
        p_ref[pl.ds(REACH + i, depth, stride=width), :] = choose(odd, near.shape, far, near).T
        p_ref[pl.ds(REACH - 1 - i, depth, stride=width), :] = choose(odd, near.shape, near, far).T


def join_kernel(levels, parts_ref, image_ref):
    width = 2 * REACH
    for source in range(parts_ref.shape[0] // (levels * width)):
        for z in range(levels):
            at = (source * levels + z) * width
            block = parts_ref[at : at + width, :]
            if source % 2 == 0:
                block = jnp.concatenate([block[REACH:], block[:REACH]], axis=0)
            image_ref[z, source * width : (source + 1) * width, :] = block


def pairs(size, first):
    left = [(i, i + 1) for i in range(first, size - 1, 2)]
    return left + [(b, a) for a, b in left]


def shards(
    pressure,
    pressure_prior,
    courant_square,
    wavelet,
    delay_steps,
    source_depth,
    receiver_depth,
    receiver_field,
):
    depth, width, length = pressure.shape
    size, cores = lax.axis_size("gx"), lax.axis_size("gy")
    near_pairs, far_pairs = pairs(size, 0), pairs(size, 1)
    rim_pairs = pairs(cores, 0)
    odd = lax.axis_index("gx") % 2
    first = jnp.where(lax.axis_index("gy") == 0, 1, 0)
    rows = lax.broadcasted_iota(jnp.int32, (8, length), 0)
    sides = jnp.where(rows == 0, odd, first).astype(F32)
    flat = (depth * width, length)
    half = jax.ShapeDtypeStruct((REACH, length, depth), F32)
    rims = jax.ShapeDtypeStruct((2 * REACH, REACH, depth), F32)
    whole = jax.ShapeDtypeStruct(flat, F32)
    square = jax.ShapeDtypeStruct((length, length), F32)
    wave = jnp.broadcast_to(wavelet[:, None], (wavelet.shape[0], length))

    def kernel(body, outs, inputs, scratch=(), name=None):
        return pl.pallas_call(
            body,
            out_shape=outs,
            in_specs=[VM] * len(inputs),
            out_specs=jax.tree.map(lambda _: VM, outs),
            scratch_shapes=list(scratch),
            compiler_params=PARAMS,
            name=name,
        )(*inputs)

    start = pressure.reshape(flat)
    near = kernel(open_near_kernel, half, (sides, start), name="open_near")
    far, edge = kernel(open_far_kernel, (half, rims), (sides, start, near), name="open_far")
    near_prior, far_prior, near_coef, far_coef, near_mark, far_mark, amp = kernel(
        tables_kernel,
        (half,) * 6 + (square,),
        (
            sides,
            wave,
            pressure_prior.reshape(flat),
            courant_square.astype(F32).reshape(flat),
            delay_steps,
            source_depth,
        ),
        name="tables",
    )
    scratch = (pltpu.VMEM((REACH, length + 16, depth), F32), pltpu.VMEM((REACH * length, depth), F32))
    pad = (pltpu.VMEM((depth + 16, length), F32),)
    receiver = receiver_field.reshape(flat)
    for step in range(STEPS):
        near_halo = lax.ppermute(near, "gx", near_pairs)
        far_halo = lax.ppermute(far, "gx", far_pairs)
        edge_in = lax.ppermute(edge, "gy", rim_pairs)
        near_next = kernel(
            functools.partial(advance_kernel, step, 0),
            half,
            (sides, near, far, near_halo, edge_in, near_prior, near_coef, near_mark, amp),
            scratch,
            f"near{step}",
        )
        far_inputs = (sides, far, near, far_halo, edge_in, far_prior, far_coef, far_mark, amp)
        if step < STEPS - 1:
            far_next, edge = kernel(
                functools.partial(advance_kernel, step, 1),
                (half, rims),
                far_inputs + (near_next,),
                scratch,
                f"far{step}",
            )
        else:
            part = kernel(
                image_near_kernel,
                jax.ShapeDtypeStruct((depth * REACH, length), F32),
                (sides, near_next, receiver, receiver_depth),
                pad,
                "image_near",
            )
            far_next, filtered = kernel(
                functools.partial(last_kernel, step),
                (half, whole),
                far_inputs + (receiver, receiver_depth, part),
                scratch + pad,
                f"far{step}",
            )
        near_prior, far_prior = near, far
        near, far = near_next, far_next
    levels = depth // size
    parts = lax.all_to_all(filtered, "gx", split_axis=0, concat_axis=0, tiled=True)
    final = kernel(final_kernel, whole, (sides, near, far), name="final")
    image = kernel(
        functools.partial(join_kernel, levels),
        jax.ShapeDtypeStruct((levels, size * width, length), F32),
        (parts,),
        name="join",
    )
    return final.reshape(depth, width, length), image


def solution(mesh):
    in_specs = (
        P(None, ("shots", "gx"), "gy"),
        P(None, ("shots", "gx"), "gy"),
        P(None, "gx", "gy"),
        P("shots"),
        P(("shots", "gx"), "gy"),
        P(("shots", "gx"), "gy"),
        P(("shots", "gx"), "gy"),
        P(None, ("shots", "gx"), "gy"),
    )
    out_specs = (P(None, ("shots", "gx"), "gy"), P("gx", "shots", "gy"))
    return jax.shard_map(shards, mesh=mesh, in_specs=in_specs, out_specs=out_specs, check_vma=False)
```

```python
import functools

import jax
import jax.numpy as jnp
from jax import lax
from jax.experimental import pallas as pl
from jax.experimental.pallas import tpu as pltpu
from jax.sharding import PartitionSpec as P

STEPS = 8

CENTER = -205.0 / 72.0
COEFS = (1.6, -0.2, 8.0 / 315.0, -1.0 / 560.0)
REACH = len(COEFS)
CHUNK = 32

VM = pl.BlockSpec(memory_space=pltpu.VMEM)
F32 = jnp.float32
BF16 = jnp.bfloat16
PARAMS = pltpu.CompilerParams(vmem_limit_bytes=8 * 2**20)


def choose(flag, shape, yes, no):
    return jnp.where(jnp.broadcast_to(flag, shape) > 0.5, yes, no)


def split_planes(src_ref, odd, put):
    depth = src_ref.shape[0] // (2 * REACH)
    for i in range(REACH):
        right = src_ref[pl.ds(REACH + i, depth, stride=2 * REACH), :]
        left = src_ref[pl.ds(REACH - 1 - i, depth, stride=2 * REACH), :]
        put(i, choose(odd, right.shape, left, right).T, choose(odd, right.shape, right, left).T)


def rim(plane_ref, i, first):
    length, depth = plane_ref.shape[1:]
    return choose(first, (REACH, depth), plane_ref[i, length - REACH : length, :], plane_ref[i, 0:REACH, :])


def open_near_kernel(sides_ref, p_ref, near_ref):
    def put(i, near, far):
        near_ref[i] = near

    split_planes(p_ref, sides_ref[0:1, :], put)


def open_far_kernel(sides_ref, p_ref, near_ref, far_ref, rim_ref):
    first = sides_ref[1:2, :]

    def put(i, near, far):
        far_ref[i] = far

    split_planes(p_ref, sides_ref[0:1, :], put)
    for i in range(REACH):
        rim_ref[i] = rim(near_ref, i, first)
        rim_ref[REACH + i] = rim(far_ref, i, first)


def tables_kernel(
    sides_ref, wavelet_ref, prior_ref, coef_ref, delay_ref, depth_ref,
    prior_near, prior_far, coef_near, coef_far, mark_near, mark_far, amp_ref,
):
    odd = sides_ref[0:1, :]
    length, depth = prior_near.shape[1:]

    def put_prior(i, near, far):
        prior_near[i] = near
        prior_far[i] = far

    def put_coef(i, near, far):
        coef_near[i] = near
        coef_far[i] = far

    split_planes(prior_ref, odd, put_prior)
    split_planes(coef_ref, odd, put_coef)

    def arrange(rows):
        right = [rows[REACH + i : REACH + i + 1, :] for i in range(REACH)]
        left = [rows[REACH - 1 - i : REACH - i, :] for i in range(REACH)]
        return choose(odd, rows.shape, jnp.concatenate(left + right, axis=0), jnp.concatenate(right + left, axis=0))

    delay = delay_ref[...]
    rows = []
    for step in range(STEPS):
        amplitude = jnp.zeros(delay.shape, F32)
        for w in range(wavelet_ref.shape[0]):
            wave = jnp.broadcast_to(wavelet_ref[w : w + 1, :], delay.shape)
            amplitude = jnp.where(delay + step == w, wave, amplitude)
        rows.append(arrange(amplitude))
    rows.append(arrange(depth_ref[...].astype(F32)))
    fill = jnp.zeros((length - len(rows) * 2 * REACH, length), F32)
    columns = jnp.concatenate(rows + [fill], axis=0).T
    amp_ref[...] = columns
    levels = lax.broadcasted_iota(jnp.int32, (length, depth), 1).astype(F32)
    base = STEPS * 2 * REACH
    for i in range(REACH):
        mark_near[i] = jnp.where(levels == columns[:, base + i : base + i + 1], 1.0, 0.0)
        mark_far[i] = jnp.where(levels == columns[:, base + REACH + i : base + REACH + i + 1], 1.0, 0.0)


def advance_kernel(
    step, half, sides_ref, self_ref, other_ref, halo_ref, rim_in_ref, prior_ref, coef_ref, mark_ref, amp_ref, *rest
):
    pad_ref, deep_ref = rest[-2:]
    first = sides_ref[1:2, :]
    planes, length, depth = self_ref.shape
    out_ref = rest[-3]
    for i in range(planes):
        edge = rim_in_ref[half * REACH + i]
        none = jnp.zeros_like(edge)
        pad_ref[i, 8 : 8 + length, :] = self_ref[i]
        pad_ref[i, 8 - REACH : 8, :] = choose(first, edge.shape, none, edge)
        pad_ref[i, 8 + length : 8 + length + REACH, :] = choose(first, edge.shape, edge, none)
    apart = jnp.abs(
        lax.broadcasted_iota(jnp.int32, (depth, depth), 0) - lax.broadcasted_iota(jnp.int32, (depth, depth), 1)
    )
    band = jnp.where(apart == 0, F32(3.0 * CENTER), F32(0.0))
    for k in range(1, REACH + 1):
        band = jnp.where(apart == k, F32(COEFS[k - 1]), band)
    band_high = band.astype(BF16)
    band_low = (band - band_high.astype(F32)).astype(BF16)
    flat = self_ref[...].reshape(planes * length, depth)
    high = flat.astype(BF16)
    low = (flat - high.astype(F32)).astype(BF16)
    dot = functools.partial(jnp.dot, preferred_element_type=F32)
    deep_ref[...] = dot(high, band_high) + (dot(low, band_high) + dot(high, band_low))
    for row in range(0, length, CHUNK):
        at = slice(row, row + CHUNK)
        line = [other_ref[REACH - 1 - i, at, :] for i in range(REACH)]
        line += [self_ref[i, at, :] for i in range(REACH)]
        if halo_ref is not None:
            line += [halo_ref[REACH - 1 - i, at, :] for i in range(REACH)]
        for i in range(planes):
            total = deep_ref[i * length + row : i * length + row + CHUNK, :]
            for k in range(1, REACH + 1):
                around = line[REACH + i - k]
                if REACH + i + k < len(line):
                    around = around + line[REACH + i + k]
                around = around + pad_ref[i, 8 + row - k : 8 + row - k + CHUNK, :]
                around = around + pad_ref[i, 8 + row + k : 8 + row + k + CHUNK, :]
                total = total + COEFS[k - 1] * around
            column = (step * 2 + half) * REACH + i
            out_ref[i, at, :] = (
                2.0 * line[REACH + i]
                - prior_ref[i, at, :]
                + coef_ref[i, at, :] * total
                + mark_ref[i, at, :] * amp_ref[at, column : column + 1]
            )


def inner_kernel(step, half, sides_ref, self_ref, other_ref, *rest):
    advance_kernel(step, half, sides_ref, self_ref, other_ref, None, *rest)


def add_halo(base_ref, coef_ref, halo_ref, out_ref):
    planes, length, _ = base_ref.shape
    for row in range(0, length, CHUNK):
        at = slice(row, row + CHUNK)
        for i in range(planes):
            for k in range(REACH - i, REACH + 1):
                term = COEFS[k - 1] * halo_ref[2 * REACH - 1 - i - k, at, :]
                total = term if k == REACH - i else total + term
            out_ref[i, at, :] = base_ref[i, at, :] + coef_ref[i, at, :] * total


def outer_kernel(sides_ref, base_ref, coef_ref, halo_ref, near_ref, out_ref, rim_ref):
    first = sides_ref[1:2, :]
    add_halo(base_ref, coef_ref, halo_ref, out_ref)
    for i in range(REACH):
        rim_ref[i] = rim(near_ref, i, first)
        rim_ref[REACH + i] = rim(out_ref, i, first)


def image_half(is_near, sides_ref, half_ref, receiver_ref, receiver_depth_ref, image_ref, pad_ref, row, stride):
    odd = sides_ref[0:1, :]
    length, depth = half_ref.shape[1:]
    width = 2 * REACH
    levels = lax.broadcasted_iota(jnp.int32, (depth, length), 0).astype(F32)
    start = receiver_depth_ref[...].astype(F32)
    pad_ref[0:8, :] = jnp.zeros((8, length), F32)
    pad_ref[8 + depth : 16 + depth, :] = jnp.zeros((8, length), F32)
    for j in range(REACH):
        rising, falling = half_ref[j], half_ref[REACH - 1 - j]
        low = receiver_ref[pl.ds(j, depth, stride=width), :]
        high = receiver_ref[pl.ds(REACH + j, depth, stride=width), :]
        start_low, start_high = start[j : j + 1, :], start[REACH + j : REACH + j + 1, :]
        if is_near:
            field = choose(odd, rising.shape, falling, rising).T
            receiver = choose(odd, low.shape, low, high)
            begin = choose(odd, start_low.shape, start_low, start_high)
        else:
            field = choose(odd, rising.shape, rising, falling).T
            receiver = choose(odd, low.shape, high, low)
            begin = choose(odd, start_low.shape, start_high, start_low)
        begin = jnp.broadcast_to(begin, levels.shape)
        product = field * jnp.where(levels >= begin, receiver, jnp.zeros_like(receiver))
        pad_ref[8 : 8 + depth, :] = product
        image_ref[pl.ds(row + j, depth, stride=stride), :] = (
            2.0 * product - pad_ref[7 : 7 + depth, :] - pad_ref[9 : 9 + depth, :]
        )


def image_near_kernel(sides_ref, near_ref, receiver_ref, receiver_depth_ref, image_ref, pad_ref):
    image_half(True, sides_ref, near_ref, receiver_ref, receiver_depth_ref, image_ref, pad_ref, 0, REACH)


def last_kernel(
    sides_ref, base_ref, coef_ref, halo_ref, receiver_ref, receiver_depth_ref, part_ref, far_ref, image_ref, pad_ref
):
    add_halo(base_ref, coef_ref, halo_ref, far_ref)
    width = 2 * REACH
    depth = part_ref.shape[0] // REACH
    image_half(False, sides_ref, far_ref, receiver_ref, receiver_depth_ref, image_ref, pad_ref, REACH, width)
    for j in range(REACH):
        image_ref[pl.ds(j, depth, stride=width), :] = part_ref[pl.ds(j, depth, stride=REACH), :]


def final_kernel(sides_ref, near_ref, far_ref, p_ref):
    odd = sides_ref[0:1, :]
    width = 2 * REACH
    depth = p_ref.shape[0] // width
    for i in range(REACH):
        near, far = near_ref[i], far_ref[i]
        p_ref[pl.ds(REACH + i, depth, stride=width), :] = choose(odd, near.shape, far, near).T
        p_ref[pl.ds(REACH - 1 - i, depth, stride=width), :] = choose(odd, near.shape, near, far).T


def join_kernel(levels, parts_ref, image_ref):
    width = 2 * REACH
    for source in range(parts_ref.shape[0] // (levels * width)):
        for z in range(levels):
            at = (source * levels + z) * width
            block = parts_ref[at : at + width, :]
            if source % 2 == 0:
                block = jnp.concatenate([block[REACH:], block[:REACH]], axis=0)
            image_ref[z, source * width : (source + 1) * width, :] = block


def pairs(size, first):
    left = [(i, i + 1) for i in range(first, size - 1, 2)]
    return left + [(b, a) for a, b in left]


def shards(
    pressure,
    pressure_prior,
    courant_square,
    wavelet,
    delay_steps,
    source_depth,
    receiver_depth,
    receiver_field,
):
    depth, width, length = pressure.shape
    size, cores = lax.axis_size("gx"), lax.axis_size("gy")
    near_pairs, far_pairs = pairs(size, 0), pairs(size, 1)
    rim_pairs = pairs(cores, 0)
    odd = lax.axis_index("gx") % 2
    first = jnp.where(lax.axis_index("gy") == 0, 1, 0)
    rows = lax.broadcasted_iota(jnp.int32, (8, length), 0)
    sides = jnp.where(rows == 0, odd, first).astype(F32)
    flat = (depth * width, length)
    half = jax.ShapeDtypeStruct((REACH, length, depth), F32)
    rims = jax.ShapeDtypeStruct((2 * REACH, REACH, depth), F32)
    whole = jax.ShapeDtypeStruct(flat, F32)
    square = jax.ShapeDtypeStruct((length, length), F32)
    wave = jnp.broadcast_to(wavelet[:, None], (wavelet.shape[0], length))

    def kernel(body, outs, inputs, scratch=(), name=None):
        return pl.pallas_call(
            body,
            out_shape=outs,
            in_specs=[VM] * len(inputs),
            out_specs=jax.tree.map(lambda _: VM, outs),
            scratch_shapes=list(scratch),
            compiler_params=PARAMS,
            name=name,
        )(*inputs)

    start = pressure.reshape(flat)
    near = kernel(open_near_kernel, half, (sides, start), name="open_near")
    far, edge = kernel(open_far_kernel, (half, rims), (sides, start, near), name="open_far")
    near_prior, far_prior, near_coef, far_coef, near_mark, far_mark, amp = kernel(
        tables_kernel,
        (half,) * 6 + (square,),
        (
            sides,
            wave,
            pressure_prior.reshape(flat),
            courant_square.astype(F32).reshape(flat),
            delay_steps,
            source_depth,
        ),
        name="tables",
    )
    scratch = (pltpu.VMEM((REACH, length + 16, depth), F32), pltpu.VMEM((REACH * length, depth), F32))
    pad = (pltpu.VMEM((depth + 16, length), F32),)
    receiver = receiver_field.reshape(flat)
    for step in range(STEPS):
        near_halo = lax.ppermute(near, "gx", near_pairs)
        far_halo = lax.ppermute(far, "gx", far_pairs)
        edge_in = lax.ppermute(edge, "gy", rim_pairs)
        near_next = kernel(
            functools.partial(advance_kernel, step, 0),
            half,
            (sides, near, far, near_halo, edge_in, near_prior, near_coef, near_mark, amp),
            scratch,
            f"near{step}",
        )
        base = kernel(
            functools.partial(inner_kernel, step, 1),
            half,
            (sides, far, near, edge_in, far_prior, far_coef, far_mark, amp, near_next),
            scratch,
            f"inner{step}",
        )
        if step < STEPS - 1:
            far_next, edge = kernel(
                outer_kernel, (half, rims), (sides, base, far_coef, far_halo, near_next), name=f"far{step}"
            )
        else:
            part = kernel(
                image_near_kernel,
                jax.ShapeDtypeStruct((depth * REACH, length), F32),
                (sides, near_next, receiver, receiver_depth),
                pad,
                "image_near",
            )
            far_next, filtered = kernel(
                last_kernel,
                (half, whole),
                (sides, base, far_coef, far_halo, receiver, receiver_depth, part),
                pad,
                f"far{step}",
            )
        near_prior, far_prior = near, far
        near, far = near_next, far_next
    levels = depth // size
    parts = lax.all_to_all(filtered, "gx", split_axis=0, concat_axis=0, tiled=True)
    final = kernel(final_kernel, whole, (sides, near, far), name="final")
    image = kernel(
        functools.partial(join_kernel, levels),
        jax.ShapeDtypeStruct((levels, size * width, length), F32),
        (parts,),
        name="join",
    )
    return final.reshape(depth, width, length), image


def solution(mesh):
    in_specs = (
        P(None, ("shots", "gx"), "gy"),
        P(None, ("shots", "gx"), "gy"),
        P(None, "gx", "gy"),
        P("shots"),
        P(("shots", "gx"), "gy"),
        P(("shots", "gx"), "gy"),
        P(("shots", "gx"), "gy"),
        P(None, ("shots", "gx"), "gy"),
    )
    out_specs = (P(None, ("shots", "gx"), "gy"), P("gx", "shots", "gy"))
    return jax.shard_map(shards, mesh=mesh, in_specs=in_specs, out_specs=out_specs, check_vma=False)
```

```python
import functools

import jax
import jax.numpy as jnp
from jax import lax
from jax.experimental import pallas as pl
from jax.experimental.pallas import tpu as pltpu
from jax.sharding import PartitionSpec as P


STEPS = 8

CENTER = -205.0 / 72.0
COEFS = (1.6, -0.2, 8.0 / 315.0, -1.0 / 560.0)
REACH = len(COEFS)
CHUNK = 32

VM = pl.BlockSpec(memory_space=pltpu.VMEM)
F32 = jnp.float32
BF16 = jnp.bfloat16
PARAMS = pltpu.CompilerParams(vmem_limit_bytes=8 * 2**20)


def choose(flag, shape, yes, no):
    return jnp.where(jnp.broadcast_to(flag, shape) > 0.5, yes, no)


def split_planes(src_ref, odd, put):
    depth = src_ref.shape[0] // (2 * REACH)
    for i in range(REACH):
        right = src_ref[pl.ds(REACH + i, depth, stride=2 * REACH), :]
        left = src_ref[pl.ds(REACH - 1 - i, depth, stride=2 * REACH), :]
        put(i, choose(odd, right.shape, left, right).T, choose(odd, right.shape, right, left).T)


def rim(plane_ref, i, first):
    length, depth = plane_ref.shape[1:]
    return choose(first, (REACH, depth), plane_ref[i, length - REACH : length, :], plane_ref[i, 0:REACH, :])


def open_near_kernel(sides_ref, p_ref, near_ref):
    def put(i, near, far):
        near_ref[i] = near

    split_planes(p_ref, sides_ref[0:1, :], put)


def open_far_kernel(sides_ref, p_ref, near_ref, far_ref, rim_ref):
    first = sides_ref[1:2, :]

    def put(i, near, far):
        far_ref[i] = far

    split_planes(p_ref, sides_ref[0:1, :], put)
    for i in range(REACH):
        rim_ref[i] = rim(near_ref, i, first)
        rim_ref[REACH + i] = rim(far_ref, i, first)


def tables_kernel(
    sides_ref, wavelet_ref, prior_ref, coef_ref, delay_ref, depth_ref,
    prior_near, prior_far, coef_near, coef_far, mark_near, mark_far, amp_ref,
):
    odd = sides_ref[0:1, :]
    length, depth = prior_near.shape[1:]

    def put_prior(i, near, far):
        prior_near[i] = near
        prior_far[i] = far

    def put_coef(i, near, far):
        coef_near[i] = near
        coef_far[i] = far

    split_planes(prior_ref, odd, put_prior)
    split_planes(coef_ref, odd, put_coef)

    def arrange(rows):
        right = [rows[REACH + i : REACH + i + 1, :] for i in range(REACH)]
        left = [rows[REACH - 1 - i : REACH - i, :] for i in range(REACH)]
        return choose(odd, rows.shape, jnp.concatenate(left + right, axis=0), jnp.concatenate(right + left, axis=0))

    delay = delay_ref[...]
    rows = []
    for step in range(STEPS):
        amplitude = jnp.zeros(delay.shape, F32)
        for w in range(wavelet_ref.shape[0]):
            wave = jnp.broadcast_to(wavelet_ref[w : w + 1, :], delay.shape)
            amplitude = jnp.where(delay + step == w, wave, amplitude)
        rows.append(arrange(amplitude))
    rows.append(arrange(depth_ref[...].astype(F32)))
    fill = jnp.zeros((length - len(rows) * 2 * REACH, length), F32)
    columns = jnp.concatenate(rows + [fill], axis=0).T
    amp_ref[...] = columns
    levels = lax.broadcasted_iota(jnp.int32, (length, depth), 1).astype(F32)
    base = STEPS * 2 * REACH
    for i in range(REACH):
        mark_near[i] = jnp.where(levels == columns[:, base + i : base + i + 1], 1.0, 0.0)
        mark_far[i] = jnp.where(levels == columns[:, base + REACH + i : base + REACH + i + 1], 1.0, 0.0)


def advance_kernel(
    step, half, sides_ref, self_ref, other_ref, halo_ref, rim_in_ref, prior_ref, coef_ref, mark_ref, amp_ref, *rest
):
    pad_ref, deep_ref = rest[-2:]
    first = sides_ref[1:2, :]
    planes, length, depth = self_ref.shape
    out_ref = rest[-3]
    for i in range(planes):
        edge = rim_in_ref[half * REACH + i]
        none = jnp.zeros_like(edge)
        pad_ref[i, 8 : 8 + length, :] = self_ref[i]
        pad_ref[i, 8 - REACH : 8, :] = choose(first, edge.shape, none, edge)
        pad_ref[i, 8 + length : 8 + length + REACH, :] = choose(first, edge.shape, edge, none)
    apart = jnp.abs(
        lax.broadcasted_iota(jnp.int32, (depth, depth), 0) - lax.broadcasted_iota(jnp.int32, (depth, depth), 1)
    )
    band = jnp.where(apart == 0, F32(3.0 * CENTER), F32(0.0))
    for k in range(1, REACH + 1):
        band = jnp.where(apart == k, F32(COEFS[k - 1]), band)
    band_high = band.astype(BF16)
    band_low = (band - band_high.astype(F32)).astype(BF16)
    flat = self_ref[...].reshape(planes * length, depth)
    high = flat.astype(BF16)
    low = (flat - high.astype(F32)).astype(BF16)
    dot = functools.partial(jnp.dot, preferred_element_type=F32)
    deep_ref[...] = dot(high, band_high) + (dot(low, band_high) + dot(high, band_low))
    for row in range(0, length, CHUNK):
        at = slice(row, row + CHUNK)
        line = [other_ref[REACH - 1 - i, at, :] for i in range(REACH)]
        line += [self_ref[i, at, :] for i in range(REACH)]
        if halo_ref is not None:
            line += [halo_ref[REACH - 1 - i, at, :] for i in range(REACH)]
        for i in range(planes):
            total = deep_ref[i * length + row : i * length + row + CHUNK, :]
            for k in range(1, REACH + 1):
                around = line[REACH + i - k]
                if REACH + i + k < len(line):
                    around = around + line[REACH + i + k]
                around = around + pad_ref[i, 8 + row - k : 8 + row - k + CHUNK, :]
                around = around + pad_ref[i, 8 + row + k : 8 + row + k + CHUNK, :]
                total = total + COEFS[k - 1] * around
            column = (step * 2 + half) * REACH + i
            out_ref[i, at, :] = (
                2.0 * line[REACH + i]
                - prior_ref[i, at, :]
                + coef_ref[i, at, :] * total
                + mark_ref[i, at, :] * amp_ref[at, column : column + 1]
            )


def inner_kernel(step, half, sides_ref, self_ref, other_ref, *rest):
    advance_kernel(step, half, sides_ref, self_ref, other_ref, None, *rest)


def add_halo(base_ref, coef_ref, halo_ref, out_ref):
    planes, length, _ = base_ref.shape
    for row in range(0, length, CHUNK):
        at = slice(row, row + CHUNK)
        for i in range(planes):
            for k in range(REACH - i, REACH + 1):
                term = COEFS[k - 1] * halo_ref[2 * REACH - 1 - i - k, at, :]
                total = term if k == REACH - i else total + term
            out_ref[i, at, :] = base_ref[i, at, :] + coef_ref[i, at, :] * total


def outer_kernel(sides_ref, base_ref, coef_ref, halo_ref, near_ref, out_ref, rim_ref):
    first = sides_ref[1:2, :]
    add_halo(base_ref, coef_ref, halo_ref, out_ref)
    for i in range(REACH):
        rim_ref[i] = rim(near_ref, i, first)
        rim_ref[REACH + i] = rim(out_ref, i, first)


def image_half(is_near, sides_ref, half_ref, receiver_ref, receiver_depth_ref, image_ref, pad_ref, row, stride):
    odd = sides_ref[0:1, :]
    length, depth = half_ref.shape[1:]
    width = 2 * REACH
    levels = lax.broadcasted_iota(jnp.int32, (depth, length), 0).astype(F32)
    start = receiver_depth_ref[...].astype(F32)
    pad_ref[0:8, :] = jnp.zeros((8, length), F32)
    pad_ref[8 + depth : 16 + depth, :] = jnp.zeros((8, length), F32)
    for j in range(REACH):
        rising, falling = half_ref[j], half_ref[REACH - 1 - j]
        low = receiver_ref[pl.ds(j, depth, stride=width), :]
        high = receiver_ref[pl.ds(REACH + j, depth, stride=width), :]
        start_low, start_high = start[j : j + 1, :], start[REACH + j : REACH + j + 1, :]
        if is_near:
            field = choose(odd, rising.shape, falling, rising).T
            receiver = choose(odd, low.shape, low, high)
            begin = choose(odd, start_low.shape, start_low, start_high)
        else:
            field = choose(odd, rising.shape, rising, falling).T
            receiver = choose(odd, low.shape, high, low)
            begin = choose(odd, start_low.shape, start_high, start_low)
        begin = jnp.broadcast_to(begin, levels.shape)
        product = field * jnp.where(levels >= begin, receiver, jnp.zeros_like(receiver))
        pad_ref[8 : 8 + depth, :] = product
        image_ref[pl.ds(row + j, depth, stride=stride), :] = (
            2.0 * product - pad_ref[7 : 7 + depth, :] - pad_ref[9 : 9 + depth, :]
        )


def image_near_kernel(sides_ref, near_ref, receiver_ref, receiver_depth_ref, image_ref, pad_ref):
    image_half(True, sides_ref, near_ref, receiver_ref, receiver_depth_ref, image_ref, pad_ref, 0, REACH)


def last_kernel(
    sides_ref, base_ref, coef_ref, halo_ref, receiver_ref, receiver_depth_ref, part_ref, far_ref, image_ref, pad_ref
):
    add_halo(base_ref, coef_ref, halo_ref, far_ref)
    width = 2 * REACH
    depth = part_ref.shape[0] // REACH
    image_half(False, sides_ref, far_ref, receiver_ref, receiver_depth_ref, image_ref, pad_ref, REACH, width)
    for j in range(REACH):
        image_ref[pl.ds(j, depth, stride=width), :] = part_ref[pl.ds(j, depth, stride=REACH), :]


def final_kernel(sides_ref, near_ref, far_ref, p_ref):
    odd = sides_ref[0:1, :]
    width = 2 * REACH
    depth = p_ref.shape[0] // width
    for i in range(REACH):
        near, far = near_ref[i], far_ref[i]
        p_ref[pl.ds(REACH + i, depth, stride=width), :] = choose(odd, near.shape, far, near).T
        p_ref[pl.ds(REACH - 1 - i, depth, stride=width), :] = choose(odd, near.shape, near, far).T


def join_kernel(levels, parts_ref, image_ref):
    width = 2 * REACH
    for source in range(parts_ref.shape[0] // (levels * width)):
        for z in range(levels):
            at = (source * levels + z) * width
            block = parts_ref[at : at + width, :]
            if source % 2 == 0:
                block = jnp.concatenate([block[REACH:], block[:REACH]], axis=0)
            image_ref[z, source * width : (source + 1) * width, :] = block


def pairs(size, first):
    left = [(i, i + 1) for i in range(first, size - 1, 2)]
    return left + [(b, a) for a, b in left]


def shards(
    pressure,
    pressure_prior,
    courant_square,
    wavelet,
    delay_steps,
    source_depth,
    receiver_depth,
    receiver_field,
):
    depth, width, length = pressure.shape
    size, cores = lax.axis_size("gx"), lax.axis_size("gy")
    near_pairs, far_pairs = pairs(size, 0), pairs(size, 1)
    rim_pairs = pairs(cores, 0)
    odd = lax.axis_index("gx") % 2
    first = jnp.where(lax.axis_index("gy") == 0, 1, 0)
    rows = lax.broadcasted_iota(jnp.int32, (8, length), 0)
    sides = jnp.where(rows == 0, odd, first).astype(F32)
    flat = (depth * width, length)
    half = jax.ShapeDtypeStruct((REACH, length, depth), F32)
    rims = jax.ShapeDtypeStruct((2 * REACH, REACH, depth), F32)
    whole = jax.ShapeDtypeStruct(flat, F32)
    square = jax.ShapeDtypeStruct((length, length), F32)
    wave = jnp.broadcast_to(wavelet[:, None], (wavelet.shape[0], length))

    def kernel(body, outs, inputs, scratch=()):
        return pl.pallas_call(
            body,
            out_shape=outs,
            in_specs=[VM] * len(inputs),
            out_specs=jax.tree.map(lambda _: VM, outs),
            scratch_shapes=list(scratch),
            compiler_params=PARAMS,
        )(*inputs)

    start = pressure.reshape(flat)
    near = kernel(open_near_kernel, half, (sides, start))
    far, edge = kernel(open_far_kernel, (half, rims), (sides, start, near))
    near_prior, far_prior, near_coef, far_coef, near_mark, far_mark, amp = kernel(
        tables_kernel,
        (half,) * 6 + (square,),
        (
            sides,
            wave,
            pressure_prior.reshape(flat),
            courant_square.astype(F32).reshape(flat),
            delay_steps,
            source_depth,
        ),
    )
    scratch = (pltpu.VMEM((REACH, length + 16, depth), F32), pltpu.VMEM((REACH * length, depth), F32))
    pad = (pltpu.VMEM((depth + 16, length), F32),)
    receiver = receiver_field.reshape(flat)
    for step in range(STEPS):
        near_halo = lax.ppermute(near, "gx", near_pairs)
        edge_in = lax.ppermute(edge, "gy", rim_pairs)
        far_halo = lax.ppermute(far, "gx", far_pairs)
        near_next = kernel(
            functools.partial(advance_kernel, step, 0),
            half,
            (sides, near, far, near_halo, edge_in, near_prior, near_coef, near_mark, amp),
            scratch,
        )
        base = kernel(
            functools.partial(inner_kernel, step, 1),
            half,
            (sides, far, near, edge_in, far_prior, far_coef, far_mark, amp, near_next),
            scratch,
        )
        if step < STEPS - 1:
            far_next, edge = kernel(outer_kernel, (half, rims), (sides, base, far_coef, far_halo, near_next))
        else:
            part = kernel(
                image_near_kernel,
                jax.ShapeDtypeStruct((depth * REACH, length), F32),
                (sides, near_next, receiver, receiver_depth),
                pad,
            )
            far_next, filtered = kernel(
                last_kernel, (half, whole), (sides, base, far_coef, far_halo, receiver, receiver_depth, part), pad
            )
        near_prior, far_prior = near, far
        near, far = near_next, far_next
    levels = depth // size
    parts = lax.all_to_all(filtered, "gx", split_axis=0, concat_axis=0, tiled=True)
    final = kernel(final_kernel, whole, (sides, near, far))
    image = kernel(
        functools.partial(join_kernel, levels), jax.ShapeDtypeStruct((levels, size * width, length), F32), (parts,)
    )
    return final.reshape(depth, width, length), image


def solution(mesh):
    in_specs = (
        P(None, ("shots", "gx"), "gy"),
        P(None, ("shots", "gx"), "gy"),
        P(None, "gx", "gy"),
        P("shots"),
        P(("shots", "gx"), "gy"),
        P(("shots", "gx"), "gy"),
        P(("shots", "gx"), "gy"),
        P(None, ("shots", "gx"), "gy"),
    )
    out_specs = (P(None, ("shots", "gx"), "gy"), P("gx", "shots", "gy"))
    return jax.shard_map(shards, mesh=mesh, in_specs=in_specs, out_specs=out_specs, check_vma=False)
```

```python
import functools

import jax
import jax.numpy as jnp
from jax import lax
from jax.experimental import pallas as pl
from jax.experimental.pallas import tpu as pltpu
from jax.sharding import PartitionSpec as P

STEPS = 8

CENTER = -205.0 / 72.0
COEFS = (1.6, -0.2, 8.0 / 315.0, -1.0 / 560.0)
REACH = len(COEFS)
CHUNK = 32

VM = pl.BlockSpec(memory_space=pltpu.VMEM)
F32 = jnp.float32
BF16 = jnp.bfloat16
PARAMS = pltpu.CompilerParams(vmem_limit_bytes=8 * 2**20)


def choose(flag, shape, yes, no):
    return jnp.where(jnp.broadcast_to(flag, shape) > 0.5, yes, no)


def split_planes(src_ref, odd, put):
    depth = src_ref.shape[0] // (2 * REACH)
    for i in range(REACH):
        right = src_ref[pl.ds(REACH + i, depth, stride=2 * REACH), :]
        left = src_ref[pl.ds(REACH - 1 - i, depth, stride=2 * REACH), :]
        put(i, choose(odd, right.shape, left, right).T, choose(odd, right.shape, right, left).T)


def rim(plane_ref, i, first):
    length, depth = plane_ref.shape[1:]
    return choose(first, (REACH, depth), plane_ref[i, length - REACH : length, :], plane_ref[i, 0:REACH, :])


def open_near_kernel(sides_ref, p_ref, near_ref):
    def put(i, near, far):
        near_ref[i] = near

    split_planes(p_ref, sides_ref[0:1, :], put)


def open_far_kernel(sides_ref, p_ref, near_ref, far_ref, rim_ref):
    first = sides_ref[1:2, :]

    def put(i, near, far):
        far_ref[i] = far

    split_planes(p_ref, sides_ref[0:1, :], put)
    for i in range(REACH):
        rim_ref[i] = rim(near_ref, i, first)
        rim_ref[REACH + i] = rim(far_ref, i, first)


def tables_kernel(
    sides_ref, wavelet_ref, prior_ref, coef_ref, delay_ref, depth_ref,
    prior_near, prior_far, coef_near, coef_far, mark_near, mark_far, amp_ref,
):
    odd = sides_ref[0:1, :]
    length, depth = prior_near.shape[1:]

    def put_prior(i, near, far):
        prior_near[i] = near
        prior_far[i] = far

    def put_coef(i, near, far):
        coef_near[i] = near
        coef_far[i] = far

    split_planes(prior_ref, odd, put_prior)
    split_planes(coef_ref, odd, put_coef)

    def arrange(rows):
        right = [rows[REACH + i : REACH + i + 1, :] for i in range(REACH)]
        left = [rows[REACH - 1 - i : REACH - i, :] for i in range(REACH)]
        return choose(odd, rows.shape, jnp.concatenate(left + right, axis=0), jnp.concatenate(right + left, axis=0))

    delay = delay_ref[...]
    rows = []
    for step in range(STEPS):
        amplitude = jnp.zeros(delay.shape, F32)
        for w in range(wavelet_ref.shape[0]):
            wave = jnp.broadcast_to(wavelet_ref[w : w + 1, :], delay.shape)
            amplitude = jnp.where(delay + step == w, wave, amplitude)
        rows.append(arrange(amplitude))
    rows.append(arrange(depth_ref[...].astype(F32)))
    fill = jnp.zeros((length - len(rows) * 2 * REACH, length), F32)
    columns = jnp.concatenate(rows + [fill], axis=0).T
    amp_ref[...] = columns
    levels = lax.broadcasted_iota(jnp.int32, (length, depth), 1).astype(F32)
    base = STEPS * 2 * REACH
    for i in range(REACH):
        mark_near[i] = jnp.where(levels == columns[:, base + i : base + i + 1], 1.0, 0.0)
        mark_far[i] = jnp.where(levels == columns[:, base + REACH + i : base + REACH + i + 1], 1.0, 0.0)


def advance_kernel(
    step, half, sides_ref, self_ref, other_ref, halo_ref, rim_in_ref, prior_ref, coef_ref, mark_ref, amp_ref, *rest
):
    pad_ref, deep_ref = rest[-2:]
    first = sides_ref[1:2, :]
    planes, length, depth = self_ref.shape
    out_ref = rest[-3]
    for i in range(planes):
        edge = rim_in_ref[half * REACH + i]
        none = jnp.zeros_like(edge)
        pad_ref[i, 8 : 8 + length, :] = self_ref[i]
        pad_ref[i, 8 - REACH : 8, :] = choose(first, edge.shape, none, edge)
        pad_ref[i, 8 + length : 8 + length + REACH, :] = choose(first, edge.shape, edge, none)
    apart = jnp.abs(
        lax.broadcasted_iota(jnp.int32, (depth, depth), 0) - lax.broadcasted_iota(jnp.int32, (depth, depth), 1)
    )
    band = jnp.where(apart == 0, F32(3.0 * CENTER), F32(0.0))
    for k in range(1, REACH + 1):
        band = jnp.where(apart == k, F32(COEFS[k - 1]), band)
    band_high = band.astype(BF16)
    band_low = (band - band_high.astype(F32)).astype(BF16)
    flat = self_ref[...].reshape(planes * length, depth)
    high = flat.astype(BF16)
    low = (flat - high.astype(F32)).astype(BF16)
    dot = functools.partial(jnp.dot, preferred_element_type=F32)
    deep_ref[...] = dot(high, band_high) + (dot(low, band_high) + dot(high, band_low))
    for row in range(0, length, CHUNK):
        at = slice(row, row + CHUNK)
        line = [other_ref[REACH - 1 - i, at, :] for i in range(REACH)]
        line += [self_ref[i, at, :] for i in range(REACH)]
        if halo_ref is not None:
            line += [halo_ref[REACH - 1 - i, at, :] for i in range(REACH)]
        for i in range(planes):
            total = deep_ref[i * length + row : i * length + row + CHUNK, :]
            for k in range(1, REACH + 1):
                around = line[REACH + i - k]
                if REACH + i + k < len(line):
                    around = around + line[REACH + i + k]
                around = around + pad_ref[i, 8 + row - k : 8 + row - k + CHUNK, :]
                around = around + pad_ref[i, 8 + row + k : 8 + row + k + CHUNK, :]
                total = total + COEFS[k - 1] * around
            column = (step * 2 + half) * REACH + i
            out_ref[i, at, :] = (
                2.0 * line[REACH + i]
                - prior_ref[i, at, :]
                + coef_ref[i, at, :] * total
                + mark_ref[i, at, :] * amp_ref[at, column : column + 1]
            )


def inner_kernel(step, half, sides_ref, self_ref, other_ref, *rest):
    advance_kernel(step, half, sides_ref, self_ref, other_ref, None, *rest)


def add_halo(base_ref, coef_ref, halo_ref, out_ref):
    planes, length, _ = base_ref.shape
    for row in range(0, length, CHUNK):
        at = slice(row, row + CHUNK)
        for i in range(planes):
            for k in range(REACH - i, REACH + 1):
                term = COEFS[k - 1] * halo_ref[2 * REACH - 1 - i - k, at, :]
                total = term if k == REACH - i else total + term
            out_ref[i, at, :] = base_ref[i, at, :] + coef_ref[i, at, :] * total


def outer_kernel(sides_ref, base_ref, coef_ref, halo_ref, near_ref, out_ref, rim_ref):
    first = sides_ref[1:2, :]
    add_halo(base_ref, coef_ref, halo_ref, out_ref)
    for i in range(REACH):
        rim_ref[i] = rim(near_ref, i, first)
        rim_ref[REACH + i] = rim(out_ref, i, first)


def image_half(is_near, sides_ref, half_ref, receiver_ref, receiver_depth_ref, image_ref, pad_ref, row, stride):
    odd = sides_ref[0:1, :]
    length, depth = half_ref.shape[1:]
    width = 2 * REACH
    levels = lax.broadcasted_iota(jnp.int32, (depth, length), 0).astype(F32)
    start = receiver_depth_ref[...].astype(F32)
    pad_ref[0:8, :] = jnp.zeros((8, length), F32)
    pad_ref[8 + depth : 16 + depth, :] = jnp.zeros((8, length), F32)
    for j in range(REACH):
        rising, falling = half_ref[j], half_ref[REACH - 1 - j]
        low = receiver_ref[pl.ds(j, depth, stride=width), :]
        high = receiver_ref[pl.ds(REACH + j, depth, stride=width), :]
        start_low, start_high = start[j : j + 1, :], start[REACH + j : REACH + j + 1, :]
        if is_near:
            field = choose(odd, rising.shape, falling, rising).T
            receiver = choose(odd, low.shape, low, high)
            begin = choose(odd, start_low.shape, start_low, start_high)
        else:
            field = choose(odd, rising.shape, rising, falling).T
            receiver = choose(odd, low.shape, high, low)
            begin = choose(odd, start_low.shape, start_high, start_low)
        begin = jnp.broadcast_to(begin, levels.shape)
        product = field * jnp.where(levels >= begin, receiver, jnp.zeros_like(receiver))
        pad_ref[8 : 8 + depth, :] = product
        image_ref[pl.ds(row + j, depth, stride=stride), :] = (
            2.0 * product - pad_ref[7 : 7 + depth, :] - pad_ref[9 : 9 + depth, :]
        )


def image_near_kernel(sides_ref, near_ref, receiver_ref, receiver_depth_ref, image_ref, pad_ref):
    image_half(True, sides_ref, near_ref, receiver_ref, receiver_depth_ref, image_ref, pad_ref, 0, REACH)


def last_kernel(
    sides_ref, base_ref, coef_ref, halo_ref, receiver_ref, receiver_depth_ref, part_ref, far_ref, image_ref, pad_ref
):
    add_halo(base_ref, coef_ref, halo_ref, far_ref)
    width = 2 * REACH
    depth = part_ref.shape[0] // REACH
    image_half(False, sides_ref, far_ref, receiver_ref, receiver_depth_ref, image_ref, pad_ref, REACH, width)
    for j in range(REACH):
        image_ref[pl.ds(j, depth, stride=width), :] = part_ref[pl.ds(j, depth, stride=REACH), :]


def close_kernel(levels, sides_ref, parts_ref, near_ref, far_ref, p_ref, image_ref):
    odd = sides_ref[0:1, :]
    width = 2 * REACH
    depth = p_ref.shape[0] // width
    for i in range(REACH):
        near, far = near_ref[i], far_ref[i]
        p_ref[pl.ds(REACH + i, depth, stride=width), :] = choose(odd, near.shape, far, near).T
        p_ref[pl.ds(REACH - 1 - i, depth, stride=width), :] = choose(odd, near.shape, near, far).T
    for source in range(parts_ref.shape[0] // (levels * width)):
        for z in range(levels):
            at = (source * levels + z) * width
            block = parts_ref[at : at + width, :]
            if source % 2 == 0:
                block = jnp.concatenate([block[REACH:], block[:REACH]], axis=0)
            image_ref[z, source * width : (source + 1) * width, :] = block


def pairs(size, first):
    left = [(i, i + 1) for i in range(first, size - 1, 2)]
    return left + [(b, a) for a, b in left]


def shards(
    pressure,
    pressure_prior,
    courant_square,
    wavelet,
    delay_steps,
    source_depth,
    receiver_depth,
    receiver_field,
):
    depth, width, length = pressure.shape
    size, cores = lax.axis_size("gx"), lax.axis_size("gy")
    near_pairs, far_pairs = pairs(size, 0), pairs(size, 1)
    rim_pairs = pairs(cores, 0)
    odd = lax.axis_index("gx") % 2
    first = jnp.where(lax.axis_index("gy") == 0, 1, 0)
    rows = lax.broadcasted_iota(jnp.int32, (8, length), 0)
    sides = jnp.where(rows == 0, odd, first).astype(F32)
    flat = (depth * width, length)
    half = jax.ShapeDtypeStruct((REACH, length, depth), F32)
    rims = jax.ShapeDtypeStruct((2 * REACH, REACH, depth), F32)
    whole = jax.ShapeDtypeStruct(flat, F32)
    square = jax.ShapeDtypeStruct((length, length), F32)
    wave = jnp.broadcast_to(wavelet[:, None], (wavelet.shape[0], length))

    def kernel(body, outs, inputs, scratch=(), name=None):
        return pl.pallas_call(
            body,
            out_shape=outs,
            in_specs=[VM] * len(inputs),
            out_specs=jax.tree.map(lambda _: VM, outs),
            scratch_shapes=list(scratch),
            compiler_params=PARAMS,
            name=name,
        )(*inputs)

    start = pressure.reshape(flat)
    near = kernel(open_near_kernel, half, (sides, start), name="open_near")
    far, edge = kernel(open_far_kernel, (half, rims), (sides, start, near), name="open_far")
    near_prior, far_prior, near_coef, far_coef, near_mark, far_mark, amp = kernel(
        tables_kernel,
        (half,) * 6 + (square,),
        (
            sides,
            wave,
            pressure_prior.reshape(flat),
            courant_square.astype(F32).reshape(flat),
            delay_steps,
            source_depth,
        ),
        name="tables",
    )
    scratch = (pltpu.VMEM((REACH, length + 16, depth), F32), pltpu.VMEM((REACH * length, depth), F32))
    pad = (pltpu.VMEM((depth + 16, length), F32),)
    receiver = receiver_field.reshape(flat)
    for step in range(STEPS):
        near_halo = lax.ppermute(near, "gx", near_pairs)
        far_halo = lax.ppermute(far, "gx", far_pairs)
        edge_in = lax.ppermute(edge, "gy", rim_pairs)
        near_next = kernel(
            functools.partial(advance_kernel, step, 0),
            half,
            (sides, near, far, near_halo, edge_in, near_prior, near_coef, near_mark, amp),
            scratch,
            f"near{step}",
        )
        base = kernel(
            functools.partial(inner_kernel, step, 1),
            half,
            (sides, far, near, edge_in, far_prior, far_coef, far_mark, amp, near_next),
            scratch,
            f"inner{step}",
        )
        if step < STEPS - 1:
            far_next, edge = kernel(
                outer_kernel, (half, rims), (sides, base, far_coef, far_halo, near_next), name=f"far{step}"
            )
        else:
            part = kernel(
                image_near_kernel,
                jax.ShapeDtypeStruct((depth * REACH, length), F32),
                (sides, near_next, receiver, receiver_depth),
                pad,
                "image_near",
            )
            far_next, filtered = kernel(
                last_kernel,
                (half, whole),
                (sides, base, far_coef, far_halo, receiver, receiver_depth, part),
                pad,
                f"far{step}",
            )
        near_prior, far_prior = near, far
        near, far = near_next, far_next
    levels = depth // size
    parts = lax.all_to_all(filtered, "gx", split_axis=0, concat_axis=0, tiled=True)
    final, image = kernel(
        functools.partial(close_kernel, levels),
        (whole, jax.ShapeDtypeStruct((levels, size * width, length), F32)),
        (sides, parts, near, far),
        name="close",
    )
    return final.reshape(depth, width, length), image


def solution(mesh):
    in_specs = (
        P(None, ("shots", "gx"), "gy"),
        P(None, ("shots", "gx"), "gy"),
        P(None, "gx", "gy"),
        P("shots"),
        P(("shots", "gx"), "gy"),
        P(("shots", "gx"), "gy"),
        P(("shots", "gx"), "gy"),
        P(None, ("shots", "gx"), "gy"),
    )
    out_specs = (P(None, ("shots", "gx"), "gy"), P("gx", "shots", "gy"))
    return jax.shard_map(shards, mesh=mesh, in_specs=in_specs, out_specs=out_specs, check_vma=False)
```

```python
import functools

import jax
import jax.numpy as jnp
from jax import lax
from jax.experimental import pallas as pl
from jax.experimental.pallas import tpu as pltpu
from jax.sharding import PartitionSpec as P

STEPS = 8

CENTER = -205.0 / 72.0
COEFS = (1.6, -0.2, 8.0 / 315.0, -1.0 / 560.0)
REACH = len(COEFS)
CHUNK = 32

VM = pl.BlockSpec(memory_space=pltpu.VMEM)
F32 = jnp.float32
BF16 = jnp.bfloat16
PARAMS = pltpu.CompilerParams(vmem_limit_bytes=8 * 2**20)


def choose(flag, shape, yes, no):
    return jnp.where(jnp.broadcast_to(flag, shape) > 0.5, yes, no)


def split_planes(src_ref, odd, put):
    depth = src_ref.shape[0] // (2 * REACH)
    for i in range(REACH):
        right = src_ref[pl.ds(REACH + i, depth, stride=2 * REACH), :]
        left = src_ref[pl.ds(REACH - 1 - i, depth, stride=2 * REACH), :]
        put(i, choose(odd, right.shape, left, right).T, choose(odd, right.shape, right, left).T)


def rim(plane_ref, i, first):
    length, depth = plane_ref.shape[1:]
    return choose(first, (REACH, depth), plane_ref[i, length - REACH : length, :], plane_ref[i, 0:REACH, :])


def open_near_kernel(sides_ref, p_ref, near_ref):
    def put(i, near, far):
        near_ref[i] = near

    split_planes(p_ref, sides_ref[0:1, :], put)


def open_far_kernel(sides_ref, p_ref, near_ref, far_ref, rim_ref):
    first = sides_ref[1:2, :]

    def put(i, near, far):
        far_ref[i] = far

    split_planes(p_ref, sides_ref[0:1, :], put)
    for i in range(REACH):
        rim_ref[i] = rim(near_ref, i, first)
        rim_ref[REACH + i] = rim(far_ref, i, first)


def tables_kernel(
    sides_ref, wavelet_ref, prior_ref, coef_ref, delay_ref, depth_ref,
    prior_near, prior_far, coef_near, coef_far, mark_near, mark_far, amp_ref,
):
    odd = sides_ref[0:1, :]
    length, depth = prior_near.shape[1:]

    def put_prior(i, near, far):
        prior_near[i] = near
        prior_far[i] = far

    def put_coef(i, near, far):
        coef_near[i] = near
        coef_far[i] = far

    split_planes(prior_ref, odd, put_prior)
    split_planes(coef_ref, odd, put_coef)

    def arrange(rows):
        right = [rows[REACH + i : REACH + i + 1, :] for i in range(REACH)]
        left = [rows[REACH - 1 - i : REACH - i, :] for i in range(REACH)]
        return choose(odd, rows.shape, jnp.concatenate(left + right, axis=0), jnp.concatenate(right + left, axis=0))

    delay = delay_ref[...]
    rows = []
    for step in range(STEPS):
        amplitude = jnp.zeros(delay.shape, F32)
        for w in range(wavelet_ref.shape[0]):
            wave = jnp.broadcast_to(wavelet_ref[w : w + 1, :], delay.shape)
            amplitude = jnp.where(delay + step == w, wave, amplitude)
        rows.append(arrange(amplitude))
    rows.append(arrange(depth_ref[...].astype(F32)))
    fill = jnp.zeros((length - len(rows) * 2 * REACH, length), F32)
    columns = jnp.concatenate(rows + [fill], axis=0).T
    amp_ref[...] = columns
    levels = lax.broadcasted_iota(jnp.int32, (length, depth), 1).astype(F32)
    base = STEPS * 2 * REACH
    for i in range(REACH):
        mark_near[i] = jnp.where(levels == columns[:, base + i : base + i + 1], 1.0, 0.0)
        mark_far[i] = jnp.where(levels == columns[:, base + REACH + i : base + REACH + i + 1], 1.0, 0.0)


def inner_kernel(
    step, half, sides_ref, self_ref, other_ref, rim_in_ref, prior_ref, coef_ref, mark_ref, amp_ref, *rest
):
    pad_ref, deep_ref = rest[-2:]
    first = sides_ref[1:2, :]
    planes, length, depth = self_ref.shape
    out_ref = rest[-3]
    for i in range(planes):
        edge = rim_in_ref[half * REACH + i]
        none = jnp.zeros_like(edge)
        pad_ref[i, 8 : 8 + length, :] = self_ref[i]
        pad_ref[i, 8 - REACH : 8, :] = choose(first, edge.shape, none, edge)
        pad_ref[i, 8 + length : 8 + length + REACH, :] = choose(first, edge.shape, edge, none)
    apart = jnp.abs(
        lax.broadcasted_iota(jnp.int32, (depth, depth), 0) - lax.broadcasted_iota(jnp.int32, (depth, depth), 1)
    )
    band = jnp.where(apart == 0, F32(3.0 * CENTER), F32(0.0))
    for k in range(1, REACH + 1):
        band = jnp.where(apart == k, F32(COEFS[k - 1]), band)
    band_high = band.astype(BF16)
    band_low = (band - band_high.astype(F32)).astype(BF16)
    flat = self_ref[...].reshape(planes * length, depth)
    high = flat.astype(BF16)
    low = (flat - high.astype(F32)).astype(BF16)
    dot = functools.partial(jnp.dot, preferred_element_type=F32)
    deep_ref[...] = dot(high, band_high) + (dot(low, band_high) + dot(high, band_low))
    for row in range(0, length, CHUNK):
        at = slice(row, row + CHUNK)
        line = [other_ref[REACH - 1 - i, at, :] for i in range(REACH)]
        line += [self_ref[i, at, :] for i in range(REACH)]
        for i in range(planes):
            total = deep_ref[i * length + row : i * length + row + CHUNK, :]
            for k in range(1, REACH + 1):
                around = line[REACH + i - k]
                if REACH + i + k < len(line):
                    around = around + line[REACH + i + k]
                around = around + pad_ref[i, 8 + row - k : 8 + row - k + CHUNK, :]
                around = around + pad_ref[i, 8 + row + k : 8 + row + k + CHUNK, :]
                total = total + COEFS[k - 1] * around
            column = (step * 2 + half) * REACH + i
            out_ref[i, at, :] = (
                2.0 * line[REACH + i]
                - prior_ref[i, at, :]
                + coef_ref[i, at, :] * total
                + mark_ref[i, at, :] * amp_ref[at, column : column + 1]
            )


def add_halo(base_ref, coef_ref, halo_ref, out_ref):
    planes, length, _ = base_ref.shape
    for row in range(0, length, CHUNK):
        at = slice(row, row + CHUNK)
        for i in range(planes):
            for k in range(REACH - i, REACH + 1):
                term = COEFS[k - 1] * halo_ref[2 * REACH - 1 - i - k, at, :]
                total = term if k == REACH - i else total + term
            out_ref[i, at, :] = base_ref[i, at, :] + coef_ref[i, at, :] * total


def outer_kernel(sides_ref, base_ref, coef_ref, halo_ref, near_ref, out_ref, rim_ref):
    first = sides_ref[1:2, :]
    add_halo(base_ref, coef_ref, halo_ref, out_ref)
    for i in range(REACH):
        rim_ref[i] = rim(near_ref, i, first)
        rim_ref[REACH + i] = rim(out_ref, i, first)


def image_half(is_near, sides_ref, half_ref, receiver_ref, receiver_depth_ref, image_ref, pad_ref, row, stride):
    odd = sides_ref[0:1, :]
    length, depth = half_ref.shape[1:]
    width = 2 * REACH
    levels = lax.broadcasted_iota(jnp.int32, (depth, length), 0).astype(F32)
    start = receiver_depth_ref[...].astype(F32)
    pad_ref[0:8, :] = jnp.zeros((8, length), F32)
    pad_ref[8 + depth : 16 + depth, :] = jnp.zeros((8, length), F32)
    for j in range(REACH):
        rising, falling = half_ref[j], half_ref[REACH - 1 - j]
        low = receiver_ref[pl.ds(j, depth, stride=width), :]
        high = receiver_ref[pl.ds(REACH + j, depth, stride=width), :]
        start_low, start_high = start[j : j + 1, :], start[REACH + j : REACH + j + 1, :]
        if is_near:
            field = choose(odd, rising.shape, falling, rising).T
            receiver = choose(odd, low.shape, low, high)
            begin = choose(odd, start_low.shape, start_low, start_high)
        else:
            field = choose(odd, rising.shape, rising, falling).T
            receiver = choose(odd, low.shape, high, low)
            begin = choose(odd, start_low.shape, start_high, start_low)
        begin = jnp.broadcast_to(begin, levels.shape)
        product = field * jnp.where(levels >= begin, receiver, jnp.zeros_like(receiver))
        pad_ref[8 : 8 + depth, :] = product
        image_ref[pl.ds(row + j, depth, stride=stride), :] = (
            2.0 * product - pad_ref[7 : 7 + depth, :] - pad_ref[9 : 9 + depth, :]
        )


def image_near_kernel(sides_ref, near_ref, receiver_ref, receiver_depth_ref, image_ref, pad_ref):
    image_half(True, sides_ref, near_ref, receiver_ref, receiver_depth_ref, image_ref, pad_ref, 0, REACH)


def last_kernel(
    sides_ref, base_ref, coef_ref, halo_ref, receiver_ref, receiver_depth_ref, part_ref, far_ref, image_ref, pad_ref
):
    add_halo(base_ref, coef_ref, halo_ref, far_ref)
    width = 2 * REACH
    depth = part_ref.shape[0] // REACH
    image_half(False, sides_ref, far_ref, receiver_ref, receiver_depth_ref, image_ref, pad_ref, REACH, width)
    for j in range(REACH):
        image_ref[pl.ds(j, depth, stride=width), :] = part_ref[pl.ds(j, depth, stride=REACH), :]


def close_kernel(levels, sides_ref, parts_ref, near_ref, far_ref, p_ref, image_ref):
    odd = sides_ref[0:1, :]
    width = 2 * REACH
    depth = p_ref.shape[0] // width
    for i in range(REACH):
        near, far = near_ref[i], far_ref[i]
        p_ref[pl.ds(REACH + i, depth, stride=width), :] = choose(odd, near.shape, far, near).T
        p_ref[pl.ds(REACH - 1 - i, depth, stride=width), :] = choose(odd, near.shape, near, far).T
    for source in range(parts_ref.shape[0] // (levels * width)):
        for z in range(levels):
            at = (source * levels + z) * width
            block = parts_ref[at : at + width, :]
            if source % 2 == 0:
                block = jnp.concatenate([block[REACH:], block[:REACH]], axis=0)
            image_ref[z, source * width : (source + 1) * width, :] = block


def pairs(size, first):
    left = [(i, i + 1) for i in range(first, size - 1, 2)]
    return left + [(b, a) for a, b in left]


def shards(
    pressure,
    pressure_prior,
    courant_square,
    wavelet,
    delay_steps,
    source_depth,
    receiver_depth,
    receiver_field,
):
    depth, width, length = pressure.shape
    size, cores = lax.axis_size("gx"), lax.axis_size("gy")
    near_pairs, far_pairs = pairs(size, 0), pairs(size, 1)
    rim_pairs = pairs(cores, 0)
    odd = lax.axis_index("gx") % 2
    first = jnp.where(lax.axis_index("gy") == 0, 1, 0)
    rows = lax.broadcasted_iota(jnp.int32, (8, length), 0)
    sides = jnp.where(rows == 0, odd, first).astype(F32)
    flat = (depth * width, length)
    half = jax.ShapeDtypeStruct((REACH, length, depth), F32)
    rims = jax.ShapeDtypeStruct((2 * REACH, REACH, depth), F32)
    whole = jax.ShapeDtypeStruct(flat, F32)
    square = jax.ShapeDtypeStruct((length, length), F32)
    wave = jnp.broadcast_to(wavelet[:, None], (wavelet.shape[0], length))

    def kernel(body, outs, inputs, scratch=(), name=None):
        return pl.pallas_call(
            body,
            out_shape=outs,
            in_specs=[VM] * len(inputs),
            out_specs=jax.tree.map(lambda _: VM, outs),
            scratch_shapes=list(scratch),
            compiler_params=PARAMS,
            name=name,
        )(*inputs)

    start = pressure.reshape(flat)
    near = kernel(open_near_kernel, half, (sides, start), name="open_near")
    far, edge = kernel(open_far_kernel, (half, rims), (sides, start, near), name="open_far")
    near_prior, far_prior, near_coef, far_coef, near_mark, far_mark, amp = kernel(
        tables_kernel,
        (half,) * 6 + (square,),
        (
            sides,
            wave,
            pressure_prior.reshape(flat),
            courant_square.astype(F32).reshape(flat),
            delay_steps,
            source_depth,
        ),
        name="tables",
    )
    scratch = (pltpu.VMEM((REACH, length + 16, depth), F32), pltpu.VMEM((REACH * length, depth), F32))
    pad = (pltpu.VMEM((depth + 16, length), F32),)
    receiver = receiver_field.reshape(flat)
    for step in range(STEPS):
        near_halo = lax.ppermute(near, "gx", near_pairs)
        far_halo = lax.ppermute(far, "gx", far_pairs)
        edge_in = lax.ppermute(edge, "gy", rim_pairs)
        near_base = kernel(
            functools.partial(inner_kernel, step, 0),
            half,
            (sides, near, far, edge_in, near_prior, near_coef, near_mark, amp),
            scratch,
            f"inner_near{step}",
        )
        near_next = kernel(add_halo, half, (near_base, near_coef, near_halo), name=f"near{step}")
        base = kernel(
            functools.partial(inner_kernel, step, 1),
            half,
            (sides, far, near, edge_in, far_prior, far_coef, far_mark, amp, near_next),
            scratch,
            f"inner_far{step}",
        )
        if step < STEPS - 1:
            far_next, edge = kernel(
                outer_kernel, (half, rims), (sides, base, far_coef, far_halo, near_next), name=f"far{step}"
            )
        else:
            part = kernel(
                image_near_kernel,
                jax.ShapeDtypeStruct((depth * REACH, length), F32),
                (sides, near_next, receiver, receiver_depth),
                pad,
                "image_near",
            )
            far_next, filtered = kernel(
                last_kernel,
                (half, whole),
                (sides, base, far_coef, far_halo, receiver, receiver_depth, part),
                pad,
                f"far{step}",
            )
        near_prior, far_prior = near, far
        near, far = near_next, far_next
    levels = depth // size
    parts = lax.all_to_all(filtered, "gx", split_axis=0, concat_axis=0, tiled=True)
    final, image = kernel(
        functools.partial(close_kernel, levels),
        (whole, jax.ShapeDtypeStruct((levels, size * width, length), F32)),
        (sides, parts, near, far),
        name="close",
    )
    return final.reshape(depth, width, length), image


def solution(mesh):
    in_specs = (
        P(None, ("shots", "gx"), "gy"),
        P(None, ("shots", "gx"), "gy"),
        P(None, "gx", "gy"),
        P("shots"),
        P(("shots", "gx"), "gy"),
        P(("shots", "gx"), "gy"),
        P(("shots", "gx"), "gy"),
        P(None, ("shots", "gx"), "gy"),
    )
    out_specs = (P(None, ("shots", "gx"), "gy"), P("gx", "shots", "gy"))
    return jax.shard_map(shards, mesh=mesh, in_specs=in_specs, out_specs=out_specs, check_vma=False)
```

```python
import functools

import jax
import jax.numpy as jnp
from jax import lax
from jax.experimental import pallas as pl
from jax.experimental.pallas import tpu as pltpu
from jax.sharding import PartitionSpec as P

STEPS = 8

CENTER = -205.0 / 72.0
COEFS = (1.6, -0.2, 8.0 / 315.0, -1.0 / 560.0)
REACH = len(COEFS)
CHUNK = 32

VM = pl.BlockSpec(memory_space=pltpu.VMEM)
F32 = jnp.float32
BF16 = jnp.bfloat16
PARAMS = pltpu.CompilerParams(vmem_limit_bytes=8 * 2**20)


def choose(flag, shape, yes, no):
    return jnp.where(jnp.broadcast_to(flag, shape) > 0.5, yes, no)


def split_planes(src_ref, odd, put):
    depth = src_ref.shape[0] // (2 * REACH)
    for i in range(REACH):
        right = src_ref[pl.ds(REACH + i, depth, stride=2 * REACH), :]
        left = src_ref[pl.ds(REACH - 1 - i, depth, stride=2 * REACH), :]
        put(i, choose(odd, right.shape, left, right).T, choose(odd, right.shape, right, left).T)


def rim(plane_ref, i, first):
    length, depth = plane_ref.shape[1:]
    return choose(first, (REACH, depth), plane_ref[i, length - REACH : length, :], plane_ref[i, 0:REACH, :])


def open_near_kernel(sides_ref, p_ref, near_ref):
    def put(i, near, far):
        near_ref[i] = near

    split_planes(p_ref, sides_ref[0:1, :], put)


def open_far_kernel(sides_ref, p_ref, near_ref, far_ref, rim_ref):
    first = sides_ref[1:2, :]

    def put(i, near, far):
        far_ref[i] = far

    split_planes(p_ref, sides_ref[0:1, :], put)
    for i in range(REACH):
        rim_ref[i] = rim(near_ref, i, first)
        rim_ref[REACH + i] = rim(far_ref, i, first)


def tables_kernel(
    sides_ref, wavelet_ref, prior_ref, coef_ref, delay_ref, depth_ref,
    prior_near, prior_far, coef_near, coef_far, mark_near, mark_far, amp_ref,
):
    odd = sides_ref[0:1, :]
    length, depth = prior_near.shape[1:]

    def put_prior(i, near, far):
        prior_near[i] = near
        prior_far[i] = far

    def put_coef(i, near, far):
        coef_near[i] = near
        coef_far[i] = far

    split_planes(prior_ref, odd, put_prior)
    split_planes(coef_ref, odd, put_coef)

    def arrange(rows):
        right = [rows[REACH + i : REACH + i + 1, :] for i in range(REACH)]
        left = [rows[REACH - 1 - i : REACH - i, :] for i in range(REACH)]
        return choose(odd, rows.shape, jnp.concatenate(left + right, axis=0), jnp.concatenate(right + left, axis=0))

    delay = delay_ref[...]
    rows = []
    for step in range(STEPS):
        amplitude = jnp.zeros(delay.shape, F32)
        for w in range(wavelet_ref.shape[0]):
            wave = jnp.broadcast_to(wavelet_ref[w : w + 1, :], delay.shape)
            amplitude = jnp.where(delay + step == w, wave, amplitude)
        rows.append(arrange(amplitude))
    rows.append(arrange(depth_ref[...].astype(F32)))
    fill = jnp.zeros((length - len(rows) * 2 * REACH, length), F32)
    columns = jnp.concatenate(rows + [fill], axis=0).T
    amp_ref[...] = columns
    levels = lax.broadcasted_iota(jnp.int32, (length, depth), 1).astype(F32)
    base = STEPS * 2 * REACH
    for i in range(REACH):
        mark_near[i] = jnp.where(levels == columns[:, base + i : base + i + 1], 1.0, 0.0)
        mark_far[i] = jnp.where(levels == columns[:, base + REACH + i : base + REACH + i + 1], 1.0, 0.0)


def advance_kernel(
    step, half, sides_ref, self_ref, other_ref, halo_ref, rim_in_ref, prior_ref, coef_ref, mark_ref, amp_ref, *rest
):
    pad_ref, deep_ref = rest[-2:]
    first = sides_ref[1:2, :]
    planes, length, depth = self_ref.shape
    out_ref = rest[-3]
    for i in range(planes):
        edge = rim_in_ref[half * REACH + i]
        none = jnp.zeros_like(edge)
        pad_ref[i, 8 : 8 + length, :] = self_ref[i]
        pad_ref[i, 8 - REACH : 8, :] = choose(first, edge.shape, none, edge)
        pad_ref[i, 8 + length : 8 + length + REACH, :] = choose(first, edge.shape, edge, none)
    apart = jnp.abs(
        lax.broadcasted_iota(jnp.int32, (depth, depth), 0) - lax.broadcasted_iota(jnp.int32, (depth, depth), 1)
    )
    band = jnp.where(apart == 0, F32(3.0 * CENTER), F32(0.0))
    for k in range(1, REACH + 1):
        band = jnp.where(apart == k, F32(COEFS[k - 1]), band)
    band_high = band.astype(BF16)
    band_low = (band - band_high.astype(F32)).astype(BF16)
    flat = self_ref[...].reshape(planes * length, depth)
    high = flat.astype(BF16)
    low = (flat - high.astype(F32)).astype(BF16)
    dot = functools.partial(jnp.dot, preferred_element_type=F32)
    deep_ref[...] = dot(high, band_high) + (dot(low, band_high) + dot(high, band_low))
    for row in range(0, length, CHUNK):
        at = slice(row, row + CHUNK)
        line = [other_ref[REACH - 1 - i, at, :] for i in range(REACH)]
        line += [self_ref[i, at, :] for i in range(REACH)]
        if halo_ref is not None:
            line += [halo_ref[REACH - 1 - i, at, :] for i in range(REACH)]
        for i in range(planes):
            total = deep_ref[i * length + row : i * length + row + CHUNK, :]
            for k in range(1, REACH + 1):
                around = line[REACH + i - k]
                if REACH + i + k < len(line):
                    around = around + line[REACH + i + k]
                around = around + pad_ref[i, 8 + row - k : 8 + row - k + CHUNK, :]
                around = around + pad_ref[i, 8 + row + k : 8 + row + k + CHUNK, :]
                total = total + COEFS[k - 1] * around
            column = (step * 2 + half) * REACH + i
            out_ref[i, at, :] = (
                2.0 * line[REACH + i]
                - prior_ref[i, at, :]
                + coef_ref[i, at, :] * total
                + mark_ref[i, at, :] * amp_ref[at, column : column + 1]
            )


def inner_kernel(step, half, sides_ref, self_ref, other_ref, *rest):
    advance_kernel(step, half, sides_ref, self_ref, other_ref, None, *rest)


def add_halo(base_ref, coef_ref, halo_ref, out_ref):
    planes, length, _ = base_ref.shape
    for row in range(0, length, CHUNK):
        at = slice(row, row + CHUNK)
        for i in range(planes):
            for k in range(REACH - i, REACH + 1):
                term = COEFS[k - 1] * halo_ref[2 * REACH - 1 - i - k, at, :]
                total = term if k == REACH - i else total + term
            out_ref[i, at, :] = base_ref[i, at, :] + coef_ref[i, at, :] * total


def outer_kernel(sides_ref, base_ref, coef_ref, halo_ref, near_ref, out_ref, rim_ref):
    first = sides_ref[1:2, :]
    add_halo(base_ref, coef_ref, halo_ref, out_ref)
    for i in range(REACH):
        rim_ref[i] = rim(near_ref, i, first)
        rim_ref[REACH + i] = rim(out_ref, i, first)


def image_half(is_near, sides_ref, half_ref, receiver_ref, receiver_depth_ref, image_ref, pad_ref, row, stride, keep):
    odd = sides_ref[0:1, :]
    length, depth = half_ref.shape[1:]
    width = 2 * REACH
    levels = lax.broadcasted_iota(jnp.int32, (depth, length), 0).astype(F32)
    start = receiver_depth_ref[...].astype(F32)
    pad_ref[0:8, :] = jnp.zeros((8, length), F32)
    pad_ref[8 + depth : 16 + depth, :] = jnp.zeros((8, length), F32)
    for j in range(REACH):
        rising, falling = half_ref[j], half_ref[REACH - 1 - j]
        low = receiver_ref[pl.ds(j, depth, stride=width), :]
        high = receiver_ref[pl.ds(REACH + j, depth, stride=width), :]
        start_low, start_high = start[j : j + 1, :], start[REACH + j : REACH + j + 1, :]
        if is_near:
            field = choose(odd, rising.shape, falling, rising).T
            receiver = choose(odd, low.shape, low, high)
            begin = choose(odd, start_low.shape, start_low, start_high)
        else:
            field = choose(odd, rising.shape, rising, falling).T
            receiver = choose(odd, low.shape, high, low)
            begin = choose(odd, start_low.shape, start_high, start_low)
        keep(j, field)
        begin = jnp.broadcast_to(begin, levels.shape)
        product = field * jnp.where(levels >= begin, receiver, jnp.zeros_like(receiver))
        pad_ref[8 : 8 + depth, :] = product
        image_ref[pl.ds(row + j, depth, stride=stride), :] = (
            2.0 * product - pad_ref[7 : 7 + depth, :] - pad_ref[9 : 9 + depth, :]
        )


def image_near_kernel(sides_ref, near_ref, receiver_ref, receiver_depth_ref, image_ref, field_ref, pad_ref):
    def keep(j, field):
        field_ref[j] = field

    image_half(True, sides_ref, near_ref, receiver_ref, receiver_depth_ref, image_ref, pad_ref, 0, REACH, keep)


def last_kernel(
    sides_ref, base_ref, coef_ref, halo_ref, receiver_ref, receiver_depth_ref, part_ref, field_ref,
    p_ref, image_ref, far_ref, pad_ref,
):
    add_halo(base_ref, coef_ref, halo_ref, far_ref)
    odd = sides_ref[0:1, :]
    width = 2 * REACH
    depth = part_ref.shape[0] // REACH

    def keep(j, far):
        near = field_ref[j]
        p_ref[pl.ds(j, depth, stride=width), :] = choose(odd, far.shape, near, far)
        p_ref[pl.ds(REACH + j, depth, stride=width), :] = choose(odd, far.shape, far, near)

    image_half(False, sides_ref, far_ref, receiver_ref, receiver_depth_ref, image_ref, pad_ref, REACH, width, keep)
    for j in range(REACH):
        image_ref[pl.ds(j, depth, stride=width), :] = part_ref[pl.ds(j, depth, stride=REACH), :]


def join_kernel(levels, parts_ref, image_ref):
    width = 2 * REACH
    for source in range(parts_ref.shape[0] // (levels * width)):
        for z in range(levels):
            at = (source * levels + z) * width
            block = parts_ref[at : at + width, :]
            if source % 2 == 0:
                block = jnp.concatenate([block[REACH:], block[:REACH]], axis=0)
            image_ref[z, source * width : (source + 1) * width, :] = block


def pairs(size, first):
    left = [(i, i + 1) for i in range(first, size - 1, 2)]
    return left + [(b, a) for a, b in left]


def shards(
    pressure,
    pressure_prior,
    courant_square,
    wavelet,
    delay_steps,
    source_depth,
    receiver_depth,
    receiver_field,
):
    depth, width, length = pressure.shape
    size, cores = lax.axis_size("gx"), lax.axis_size("gy")
    near_pairs, far_pairs = pairs(size, 0), pairs(size, 1)
    rim_pairs = pairs(cores, 0)
    odd = lax.axis_index("gx") % 2
    first = jnp.where(lax.axis_index("gy") == 0, 1, 0)
    rows = lax.broadcasted_iota(jnp.int32, (8, length), 0)
    sides = jnp.where(rows == 0, odd, first).astype(F32)
    flat = (depth * width, length)
    half = jax.ShapeDtypeStruct((REACH, length, depth), F32)
    rims = jax.ShapeDtypeStruct((2 * REACH, REACH, depth), F32)
    whole = jax.ShapeDtypeStruct(flat, F32)
    square = jax.ShapeDtypeStruct((length, length), F32)
    wave = jnp.broadcast_to(wavelet[:, None], (wavelet.shape[0], length))

    def kernel(body, outs, inputs, scratch=(), name=None):
        return pl.pallas_call(
            body,
            out_shape=outs,
            in_specs=[VM] * len(inputs),
            out_specs=jax.tree.map(lambda _: VM, outs),
            scratch_shapes=list(scratch),
            compiler_params=PARAMS,
            name=name,
        )(*inputs)

    start = pressure.reshape(flat)
    near = kernel(open_near_kernel, half, (sides, start), name="open_near")
    far, edge = kernel(open_far_kernel, (half, rims), (sides, start, near), name="open_far")
    near_prior, far_prior, near_coef, far_coef, near_mark, far_mark, amp = kernel(
        tables_kernel,
        (half,) * 6 + (square,),
        (
            sides,
            wave,
            pressure_prior.reshape(flat),
            courant_square.astype(F32).reshape(flat),
            delay_steps,
            source_depth,
        ),
        name="tables",
    )
    scratch = (pltpu.VMEM((REACH, length + 16, depth), F32), pltpu.VMEM((REACH * length, depth), F32))
    pad = (pltpu.VMEM((depth + 16, length), F32),)
    receiver = receiver_field.reshape(flat)
    for step in range(STEPS):
        near_halo = lax.ppermute(near, "gx", near_pairs)
        far_halo = lax.ppermute(far, "gx", far_pairs)
        edge_in = lax.ppermute(edge, "gy", rim_pairs)
        near_next = kernel(
            functools.partial(advance_kernel, step, 0),
            half,
            (sides, near, far, near_halo, edge_in, near_prior, near_coef, near_mark, amp),
            scratch,
            f"near{step}",
        )
        base = kernel(
            functools.partial(inner_kernel, step, 1),
            half,
            (sides, far, near, edge_in, far_prior, far_coef, far_mark, amp, near_next),
            scratch,
            f"inner{step}",
        )
        if step < STEPS - 1:
            far_next, edge = kernel(
                outer_kernel, (half, rims), (sides, base, far_coef, far_halo, near_next), name=f"far{step}"
            )
        else:
            part, field = kernel(
                image_near_kernel,
                (
                    jax.ShapeDtypeStruct((depth * REACH, length), F32),
                    jax.ShapeDtypeStruct((REACH, depth, length), F32),
                ),
                (sides, near_next, receiver, receiver_depth),
                pad,
                "image_near",
            )
            final, filtered = kernel(
                last_kernel,
                (whole, whole),
                (sides, base, far_coef, far_halo, receiver, receiver_depth, part, field),
                (pltpu.VMEM((REACH, length, depth), F32),) + pad,
                f"far{step}",
            )
            break
        near_prior, far_prior = near, far
        near, far = near_next, far_next
    levels = depth // size
    parts = lax.all_to_all(filtered, "gx", split_axis=0, concat_axis=0, tiled=True)
    image = kernel(
        functools.partial(join_kernel, levels),
        jax.ShapeDtypeStruct((levels, size * width, length), F32),
        (parts,),
        name="join",
    )
    return final.reshape(depth, width, length), image


def solution(mesh):
    in_specs = (
        P(None, ("shots", "gx"), "gy"),
        P(None, ("shots", "gx"), "gy"),
        P(None, "gx", "gy"),
        P("shots"),
        P(("shots", "gx"), "gy"),
        P(("shots", "gx"), "gy"),
        P(("shots", "gx"), "gy"),
        P(None, ("shots", "gx"), "gy"),
    )
    out_specs = (P(None, ("shots", "gx"), "gy"), P("gx", "shots", "gy"))
    return jax.shard_map(shards, mesh=mesh, in_specs=in_specs, out_specs=out_specs, check_vma=False)
```
